256 devices in a mesh: grp: 2 (over y_lo), row: 4 (over y_hi, core), col: 32 (over z, x).
Axes of the slice: x: 4, y: 4 (y_hi: 2, y_lo: 2; y = y_hi * 2 + y_lo), z: 8, core: 2. Of those that a mesh axis runs over, the one named last changes fastest.
Arguments:
- excitation: bfloat16 [2, 16, 32768], P('grp', None, ('row', 'col')), may hold values from -6 to 6
- panel_points: float32 [3, 32768], replicated, may hold values from 0 to 1
- panel_areas: float32 [32768], replicated, may hold values from 0.0027621358 to 0.011048543
- panel_map: int32 [32768], P(('row', 'col')), may hold values from 0 to 3
- interior_inverse: bfloat16 [32, 1024, 4, 2048], P('col', None, 'row'), may hold values from -0.0625 to 0.0625
- row_scales: float32 [32, 1024], P('col'), may hold values from 0.5 to 2
- iface_slot: int32 [32768], P(('row', 'col')), may hold values from 0 to 1
- iface_offset: int32 [32768], P(('row', 'col')), may hold values from 0 to 2047
- adjacency: int32 [4, 2], replicated, may hold values from 0 to 3, as said below
Outputs:
- traces: float32 [2, 16, 32768], P('grp', None, ('row', 'col'))
The draws below stay inside these ranges and needn't reach their ends.
Inputs may be any that keep to these rules, and one draw needn't show every extreme that they name: `adjacency`: each row lists 2 different subdomains, none equal to the row's own index.
All inputs are finite; a program needn't handle non-finite values.
Results may differ from the reference program's by a relative error of at most 0.0015.
Values may be sent and summed in bfloat16 or wider, within the bound.
A program may use at most 128 MiB of HBM per device.

```python
import math
import jax
import jax.numpy as jnp
from jax import lax

NE = 32768
SUB = 4
NADJ = 2
RHS = 16
ITERS = 4
PIECE = 256
STRIPS = 32
CL = 8
SUBN = 8192
N_ROW = 4


def draw_adjacency(key, part):

    def one_row(index):
        order = jax.random.permutation(jax.random.fold_in(key, index + 17), SUB - 1)
        return (index + 1 + order[:NADJ]) % SUB
    return jax.vmap(one_row)(jnp.arange(SUB, dtype=jnp.int32)).astype(jnp.int32)


def place_ends(values, stream_key, least, largest):
    shape = values.shape
    spot = [jax.random.randint(jax.random.fold_in(stream_key, axis), (), 0, shape[axis]) for axis in range(len(shape))]
    values = values.at[tuple(spot)].set(least)
    longest = shape.index(max(shape))
    spot[longest] = (spot[longest] + 1) % shape[longest]
    return values.at[tuple(spot)].set(largest)


def shard_levels(own_key, extent, shards, least, high):
    gain, own = 1.0, jax.random.fold_in(own_key, 6)
    for dim, blocks in shards:
        draws = jnp.exp(jax.random.uniform(jax.random.fold_in(own, dim), (blocks,), jnp.float32, least / len(shards), high / len(shards)))
        gain = gain * jnp.repeat(draws, extent[dim] // blocks).reshape([-1 if axis == dim else 1 for axis in range(len(extent))])
    return gain


def noise(own_key, shape, scale, bound, split=(), kind=jnp.bfloat16):
    drawn = jax.random.normal(own_key, shape, jnp.float32) * scale
    if len(split) > 0:
        drawn = shard_levels(own_key, shape, split, -0.22, 0.18) * drawn
    return jnp.clip(drawn, min=-bound, max=bound).astype(kind)


def setup_inputs(seed: int = 0) -> dict:
    keys = jax.random.split(jax.random.key(seed), 10)
    excitation = noise(keys[0], (2, RHS, NE), 1.0, 6.0, ((0, 2), (2, 128)))
    panel_points = jnp.clip(jax.random.uniform(keys[1], (3, NE), jnp.float32, 0.0, 1.0), 0.0, 1.0)
    panel_areas = jnp.clip(jnp.exp(jax.random.uniform(keys[2], (NE,), jnp.float32, math.log(0.0027621358), math.log(0.011048543))), 0.0027621358, 0.011048543)
    panel_map = place_ends(jax.random.randint(keys[3], (NE,), 0, SUB), jax.random.fold_in(keys[3], 1), 0, SUB - 1).astype(jnp.int32)
    interior_inverse = noise(keys[4], (STRIPS, N_ROW * PIECE, N_ROW, CL * PIECE), SUBN ** -0.5, 0.0625, ((0, 32), (2, 4)))
    row_scales = jnp.clip(jnp.exp(math.log(2.0) - 1.3862944 * jax.random.uniform(keys[5], (STRIPS, N_ROW * PIECE), jnp.float32) ** shard_levels(keys[5], (STRIPS, N_ROW * PIECE), ((0, 32),), -0.2, 0.2)), 0.5, 2.0)
    iface_slot = place_ends(jax.random.randint(keys[6], (NE,), 0, NADJ), jax.random.fold_in(keys[6], 1), 0, NADJ - 1).astype(jnp.int32)
    iface_offset = place_ends(jax.random.randint(keys[7], (NE,), 0, CL * PIECE), jax.random.fold_in(keys[7], 1), 0, (CL * PIECE) - 1).astype(jnp.int32)
    adjacency = draw_adjacency(jax.random.fold_in(keys[9], 71), 0)
    return {"excitation": excitation, "panel_points": panel_points, "panel_areas": panel_areas, "panel_map": panel_map, "interior_inverse": interior_inverse, "row_scales": row_scales, "iface_slot": iface_slot, "iface_offset": iface_offset, "adjacency": adjacency}


robin_weight = 0.5
iface_weight = 0.4
wave_number = 40.0
soften = 0.05
self_term = 0.5

def kernel_rows(panel_points, panel_areas, start, count):
    row_points = lax.dynamic_slice_in_dim(panel_points, start, count, 1)
    square = (row_points[0][:, None] - panel_points[0][None, :]) ** 2
    square = square + (row_points[1][:, None] - panel_points[1][None, :]) ** 2
    square = square + (row_points[2][:, None] - panel_points[2][None, :]) ** 2
    distance = jnp.sqrt(square)
    return (panel_areas[None, :] * jnp.cos(wave_number * distance) / (distance + soften)).astype(jnp.bfloat16)

def exterior_apply(mixed, panel_points, panel_areas):
    mixed_wide = mixed.astype(jnp.float32)
    height = min(NE, 1024)
    starts = (jnp.arange(NE // height) * height).astype(jnp.int32)

    def one_block(start):
        tile = kernel_rows(panel_points, panel_areas, start, height).astype(jnp.float32)
        return jnp.dot(mixed_wide, tile.T, precision=lax.Precision.HIGHEST)
    parts = lax.map(one_block, starts)
    far_field = jnp.transpose(parts, (1, 0, 2)).reshape(RHS, NE)
    return self_term * mixed_wide + far_field

def interior_apply(mixed, interior_inverse, row_scales):
    sub_view = mixed.astype(jnp.float32).reshape(RHS, N_ROW, SUB, CL * PIECE)

    def one_strip(strip):
        tile = lax.dynamic_index_in_dim(interior_inverse, strip, 0, keepdims=False).astype(jnp.float32)
        owned = lax.dynamic_index_in_dim(sub_view, strip // CL, 2, keepdims=False)
        result = jnp.einsum('arm,brm->ba', tile, owned, precision=lax.Precision.HIGHEST)
        scales = lax.dynamic_index_in_dim(row_scales, strip, 0, keepdims=False)
        return scales[None, :] * result
    parts = lax.map(one_strip, jnp.arange(STRIPS, dtype=jnp.int32))
    parts = parts.reshape(STRIPS, RHS, N_ROW, PIECE)
    return jnp.transpose(parts, (1, 2, 0, 3)).reshape(RHS, NE)

def reference(excitation, panel_points, panel_areas, panel_map, interior_inverse, row_scales, iface_slot, iface_offset, adjacency):
    index = jnp.arange(NE, dtype=jnp.int32)
    row_block = index // (STRIPS * PIECE)
    strip = index // PIECE % STRIPS
    sub_width = CL * PIECE
    exterior_partner = (row_block * (STRIPS * PIECE) + panel_map * sub_width + index % sub_width).astype(jnp.int32)
    neighbour = adjacency[strip // CL, iface_slot]
    interface_partner = (row_block * (STRIPS * PIECE) + neighbour * sub_width + iface_offset).astype(jnp.int32)
    base_exterior = excitation[0].astype(jnp.float32)
    base_interior = excitation[1].astype(jnp.float32)
    state_exterior = jnp.zeros((RHS, NE), jnp.float32)
    state_interior = jnp.zeros((RHS, NE), jnp.float32)
    for step in range(ITERS):
        trace_exterior = lax.optimization_barrier(state_exterior.astype(jnp.bfloat16)).astype(jnp.float32)
        trace_interior = lax.optimization_barrier(state_interior.astype(jnp.bfloat16)).astype(jnp.float32)
        far_interior = jnp.take(trace_interior, exterior_partner, axis=1)
        near_interior = jnp.take(trace_interior, interface_partner, axis=1)
        mixed_exterior = (base_exterior + robin_weight * (far_interior - trace_exterior)).astype(jnp.bfloat16)
        mixed_interior = (base_interior + robin_weight * (trace_exterior - trace_interior) + iface_weight * (near_interior - trace_interior)).astype(jnp.bfloat16)
        state_exterior = exterior_apply(mixed_exterior, panel_points, panel_areas)
        state_interior = interior_apply(mixed_interior, interior_inverse, row_scales)
    return jnp.stack([state_exterior, state_interior])
```

```python
import functools
import math

import jax
import jax.numpy as jnp
from jax import lax
from jax.experimental import pallas as pl
from jax.experimental.pallas import tpu as pltpu
from jax.sharding import PartitionSpec as P

ITERS = 4
GROUPS = 2
robin_weight = 0.5
iface_weight = 0.4
wave_number = 40.0
soften = 0.05
self_term = 0.5
KB = 32
X_CHIPS = 4

BF = jnp.bfloat16
F32 = jnp.float32
MESH = pl.DeviceIdType.MESH

COS_TERMS = (
    1.4142135381698608,
    -6.978850841522217,
    5.739460468292236,
    -1.883557915687561,
    0.3106880187988281,
)
TURNS = wave_number / (2.0 * math.pi)


def kernel(
    dims,
    exc,
    pts,
    areas,
    pmap,
    slot,
    off,
    adj,
    inv,
    scales,
    out,
    ipt,
    stage,
    kpt,
    kbuf,
    abuf,
    gbuf,
    metasend,
    metabuf,
    xmeta,
    bbuf,
    tsend,
    tbuf,
    we,
    nsend,
    nbuf,
    wi,
    acc,
    psend,
    pbuf,
    ubuf,
    asem,
    b_s,
    b_r,
    m_s,
    m_r,
    t_s,
    t_r,
    x_s,
    x_r,
    y_s,
    y_r,
):
    Z, X, R, piece, block = dims
    Zh = Z // GROUPS
    sub_width = GROUPS * X * piece
    RP = R * piece
    g = lax.axis_index("grp")
    r = lax.axis_index("row")
    c = lax.axis_index("col")
    z, x = c // X, c % X
    s = z // GROUPS
    zt = GROUPS * s + g
    parity = z % GROUPS
    me = g * R + r

    def remote(src, dst, ss, rs, dev):
        return pltpu.make_async_remote_copy(
            src_ref=src, dst_ref=dst, send_sem=ss, recv_sem=rs, device_id=dev, device_id_type=MESH
        )

    def col_of(zz, xx):
        return zz * X + xx

    barrier = pltpu.get_barrier_semaphore()
    n_partners = 0
    for flip in range(GROUPS):
        for dz in range(Z):
            if flip or dz:
                pl.semaphore_signal(
                    barrier,
                    inc=1,
                    device_id={"grp": (g + flip) % GROUPS, "row": r, "col": col_of((z + dz) % Z, x)},
                    device_id_type=MESH,
                )
                n_partners += 1
    for dx in range(1, X):
        pl.semaphore_signal(
            barrier,
            inc=1,
            device_id={"grp": g, "row": r, "col": col_of(z, (x + dx) % X)},
            device_id_type=MESH,
        )
        n_partners += 1
    for flip in range(GROUPS):
        for dr in range(1, R):
            pl.semaphore_signal(
                barrier,
                inc=1,
                device_id={"grp": (g + flip) % GROUPS, "row": (r + dr) % R, "col": c},
                device_id_type=MESH,
            )
            n_partners += 1

    inverse_copy = pltpu.make_async_copy(
        inv.at[:, pl.ds(pl.multiple_of(g * X * piece, X * piece), X * piece)], abuf, asem
    )
    inverse_copy.start()

    for rr in range(R):
        start = pl.multiple_of(rr * block + c * piece, piece)
        ipt[0:3, rr * piece : (rr + 1) * piece] = pts[:, pl.ds(start, piece)] * TURNS
    stage[...] = jnp.zeros_like(stage)

    def stage_points(p, carry):
        xx, zi = p // Zh, p % Zh
        start = pl.multiple_of(r * block + col_of(GROUPS * zi + g, xx) * piece, piece)
        stage[0:3, :] = pts[:, pl.ds(start, piece)] * TURNS
        stage[3:4, :] = areas[:, pl.ds(start, piece)] * TURNS
        kpt[pl.ds(pl.multiple_of(p * piece, piece), piece), :] = jnp.transpose(stage[...])
        return carry

    lax.fori_loop(0, X * Zh, stage_points, 0)

    per_piece = piece // KB

    def make_rows(t, carry):
        p = t // per_piece
        row = pl.multiple_of((t % per_piece) * KB, KB)
        kc = kpt[pl.ds(pl.multiple_of(t * KB, KB), KB), :]
        ix, iy, iz = ipt[0:1, :], ipt[1:2, :], ipt[2:3, :]
        dx = ix - kc[:, 0:1]
        dy = iy - kc[:, 1:2]
        dz = iz - kc[:, 2:3]
        square = dx * dx + dy * dy
        square = jnp.maximum(square + dz * dz, 1e-30)
        turns = square * lax.rsqrt(square)
        part = turns - jnp.round(turns)
        v = part * part
        h = COS_TERMS[4] * v + COS_TERMS[3]
        h = h * v + COS_TERMS[2]
        h = h * v + COS_TERMS[1]
        h = h * v + COS_TERMS[0]
        area = kc[:, 3:4]
        top = area * (h * h) - area
        value = top / (turns + soften * TURNS)
        kbuf[p // Zh, p % Zh, pl.ds(row, KB), :] = value.astype(BF)
        return carry

    quarter = X * Zh * per_piece // 4

    def make_quarter(q):
        lax.fori_loop(q * quarter, (q + 1) * quarter, make_rows, 0)

    make_quarter(0)
    pl.semaphore_wait(barrier, n_partners)

    metasend[...] = jnp.zeros_like(metasend)
    metasend[0:1, :] = pmap[...]
    metasend[1:2, :] = slot[...] * sub_width + off[...]
    b_plane = parity

    def b_copy(dz):
        return remote(
            exc.at[0],
            bbuf.at[g, z],
            b_s.at[dz],
            b_r.at[g, z],
            {"grp": b_plane, "row": r, "col": col_of((z + dz) % Z, x)},
        )

    def m_copy(dz):
        return remote(
            metasend,
            metabuf.at[z],
            m_s.at[dz],
            m_r.at[z],
            {"grp": g, "row": r, "col": col_of((z + dz) % Z, x)},
        )

    order = sorted(range(Z), key=lambda dz: -min(dz, Z - dz))
    for dz in order:
        if dz:
            b_copy(dz).start()

            @pl.when(b_plane == g)
            def _():
                m_copy(dz).start()
        else:

            @pl.when(b_plane != g)
            def _():
                b_copy(0).start()

            @pl.when(b_plane == g)
            def _():
                bbuf[g, z] = exc[0]
                metabuf[z] = metasend[...]

    make_quarter(1)

    for zi in range(Zh):
        zs = GROUPS * zi + g
        for src in range(GROUPS):

            @pl.when((zs != z) | (g != src))
            def _():
                remote(
                    bbuf.at[src, zs], bbuf.at[src, zs], b_s.at[0], b_r.at[src, zs], {"row": r}
                ).wait_recv()

        @pl.when(zs != z)
        def _():
            remote(metabuf.at[zs], metabuf.at[zs], m_s.at[0], m_r.at[zs], {"row": r}).wait_recv()

    def x_dev(dx):
        return {"grp": g, "row": r, "col": col_of(z, (x + dx) % X)}

    x_order = sorted(range(1, X), key=lambda dx: -min(dx, X - dx))

    def we_copy(k, dx):
        return remote(we.at[k, x], we.at[k, x], x_s.at[0, dx], x_r.at[k, 0, x], x_dev(dx))

    def n_copy(k, dx):
        return remote(
            nsend.at[k, (x + dx) % X], nbuf.at[k, x], x_s.at[1, dx], x_r.at[k, 1, x], x_dev(dx)
        )

    def wi_copy(k, dx):
        return remote(wi.at[k, x], wi.at[k, x], x_s.at[2, dx], x_r.at[k, 2, x], x_dev(dx))

    def xm_copy(dx):
        return remote(metabuf.at[zt], xmeta.at[x], x_s.at[1, dx], x_r.at[0, 1, x], x_dev(dx))

    def x_wait(ref, k, kind, dx):
        xs = (x + dx) % X
        remote(ref, ref, x_s.at[kind, dx], x_r.at[k, kind, xs], x_dev(dx)).wait_recv()

    for zi in range(Zh):
        we[0, x, zi] = bbuf[0, GROUPS * zi + g]
    wi[0, x] = bbuf[1, zt]
    xmeta[x] = metabuf[zt]
    for dx in x_order:
        we_copy(0, dx).start()
        xm_copy(dx).start()
        wi_copy(0, dx).start()
    make_quarter(2)

    for dx in range(1, X):
        xs = (x + dx) % X
        x_wait(xmeta.at[xs], 0, 1, dx)

    def make_gather(t, carry):
        xx, q = t // (GROUPS * GROUPS), t % (GROUPS * GROUPS)
        code = xmeta[xx, 1:2, :]
        src_x = (code // piece) % X
        src_q = code // (X * piece)
        here = jnp.where((src_x == x) & (src_q == q), code % piece, -1)
        rows = lax.broadcasted_iota(jnp.int32, (piece, piece), 0)
        hit = jnp.where(rows == here, 1.0, 0.0).astype(BF)
        gbuf[q, :, pl.ds(pl.multiple_of(xx * piece, piece), piece)] = hit
        return carry

    lax.fori_loop(0, X * GROUPS * GROUPS, make_gather, 0)
    make_quarter(3)
    inverse_copy.wait()
    for dx in range(1, X):
        x_wait(we.at[0, (x + dx) % X], 0, 0, dx)
        x_wait(wi.at[0, (x + dx) % X], 0, 2, dx)
        we_copy(0, dx).wait_send()
        xm_copy(dx).wait_send()
        wi_copy(0, dx).wait_send()
    for dz in order:
        if dz:
            b_copy(dz).wait_send()

            @pl.when(b_plane == g)
            def _():
                m_copy(dz).wait_send()
        else:

            @pl.when(b_plane != g)
            def _():
                b_copy(0).wait_send()

    def y_copy(k, kind, rr):
        return remote(
            psend.at[k, kind, rr],
            pbuf.at[k, me],
            y_s.at[kind, rr],
            y_r.at[k, me],
            {"grp": kind, "row": rr, "col": c},
        )

    def give(k, kind, rr, value):
        psend[k, kind, rr] = value
        own = (g == kind) & (r == rr)

        @pl.when(jnp.logical_not(own))
        def _():
            y_copy(k, kind, rr).start()

        @pl.when(own)
        def _():
            pbuf[k, me] = value

    def outer_part(k, xs, columns):
        total = None
        for zi in range(Zh):
            term = jnp.dot(we[k, xs, zi], kbuf[xs, zi, :, columns], preferred_element_type=F32)
            total = term if total is None else total + term
        return total

    everything = slice(None)

    def send_rows(k, xs):
        for j in range(R):
            rr = (r + 1 + j) % R
            columns = pl.ds(pl.multiple_of(rr * piece, piece), piece)
            value = acc[:, columns] + outer_part(k, xs, columns)
            own_piece = self_term * we[k, x, z // GROUPS].astype(F32)
            value = value + jnp.where((rr == r) & (parity == g), own_piece, 0.0)
            give(k, 0, rr, value)

    def inner_rows(k):
        for j in range(R):
            rr = (r + 1 + j) % R
            rows = pl.ds(pl.multiple_of(rr * piece, piece), piece)
            total = None
            for xx in range(X):
                term = lax.dot_general(
                    wi[k, xx],
                    abuf[rows, xx * piece : (xx + 1) * piece],
                    (((1,), (1,)), ((), ())),
                    preferred_element_type=F32,
                )
                total = term if total is None else total + term
            give(k, 1, rr, total)

    def collect(k):
        for src in range(GROUPS * R):

            @pl.when(src != me)
            def _():
                remote(
                    pbuf.at[k, src], pbuf.at[k, src], y_s.at[0, 0], y_r.at[k, src], {"row": r}
                ).wait_recv()

        total = pbuf[k, 0]
        for src in range(1, GROUPS * R):
            total = total + pbuf[k, src]
        scale = scales[:, pl.ds(pl.multiple_of(r * piece, piece), piece)]
        state = jnp.where(g == 0, total, scale * total)
        ubuf[...] = state
        tsend[k] = state.astype(BF)
        for kind in range(GROUPS):
            for rr in range(R):

                @pl.when((g != kind) | (r != rr))
                def _():
                    y_copy(k, kind, rr).wait_send()

    acc[...] = outer_part(0, 0, everything)
    for xx in range(1, X - 1):
        acc[...] += outer_part(0, xx, everything)
    send_rows(0, X - 1)
    inner_rows(0)
    collect(0)

    def t_copy(k, plane, dz):
        return remote(
            tsend.at[k - 1],
            tbuf.at[k, g, z],
            t_s.at[plane, dz],
            t_r.at[k, g, z],
            {"grp": plane, "row": r, "col": col_of((z + dz) % Z, x)},
        )

    def t_each(k, act):
        for dz in order:
            for plane in range(GROUPS):
                wanted = (g == 1) | (plane == parity)
                if dz == 0:
                    wanted = wanted & (plane != g)

                @pl.when(wanted)
                def _():
                    act(t_copy(k, plane, dz))

    def iteration(k, carry):
        t_each(k, lambda copy: copy.start())

        @pl.when((g == 1) | (parity == 0))
        def _():
            tbuf[k, g, z] = tsend[k - 1]

        for zz in range(Z):

            @pl.when((zz != z) | (g != 1))
            def _():
                remote(
                    tbuf.at[k, 1, zz], tbuf.at[k, 1, zz], t_s.at[0, 0], t_r.at[k, 1, zz], {"row": r}
                ).wait_recv()

        for zi in range(Zh):
            zs = GROUPS * zi + g

            @pl.when((zs != z) | (g != 0))
            def _():
                remote(
                    tbuf.at[k, 0, zs], tbuf.at[k, 0, zs], t_s.at[0, 0], t_r.at[k, 0, zs], {"row": r}
                ).wait_recv()

        for zi in range(Zh):
            zs = GROUPS * zi + g
            choice = metabuf[zs, 0:1, :]
            far = tbuf[k, 1, g].astype(F32)
            for n in range(1, Zh):
                far = jnp.where(choice == n, tbuf[k, 1, GROUPS * n + g].astype(F32), far)
            mixed = bbuf[0, zs].astype(F32) + robin_weight * (far - tbuf[k, 0, zs].astype(F32))
            we[k, x, zi] = mixed.astype(BF)
        for dx in x_order:
            we_copy(k, dx).start()

        near = None
        for j in range(GROUPS):
            for zz in range(GROUPS):
                source = tbuf[k, 1, zz].astype(F32)
                for n in range(1, Zh):
                    other = tbuf[k, 1, GROUPS * n + zz].astype(F32)
                    source = jnp.where(adj[j, s] == n, other, source)
                term = jnp.dot(
                    source.astype(BF), gbuf[j * GROUPS + zz], preferred_element_type=F32
                )
                near = term if near is None else near + term
        for xx in range(X):
            nsend[k, xx] = near[:, xx * piece : (xx + 1) * piece].astype(BF)
        for dx in x_order:
            n_copy(k, dx).start()

        acc[...] = outer_part(k, x, everything)

        near = nsend[k, x].astype(F32)
        for dx in range(1, X):
            xs = (x + dx) % X
            x_wait(nbuf.at[k, xs], k, 1, dx)
            near = near + nbuf[k, xs].astype(F32)
        inner = tbuf[k, 1, zt].astype(F32)
        outer = tbuf[k, 0, zt].astype(F32)
        mixed = (
            bbuf[1, zt].astype(F32)
            + robin_weight * (outer - inner)
            + iface_weight * (near - inner)
        )
        wi[k, x] = mixed.astype(BF)
        for dx in x_order:
            wi_copy(k, dx).start()

        x_near = x_order[::-1]
        for dx in x_near[:-1]:
            xs = (x + dx) % X
            x_wait(we.at[k, xs], k, 0, dx)
            acc[...] += outer_part(k, xs, everything)
        if X > 1:
            xs = (x + x_near[-1]) % X
            x_wait(we.at[k, xs], k, 0, x_near[-1])
        send_rows(k, xs if X > 1 else x)
        for dx in x_near:
            x_wait(wi.at[k, (x + dx) % X], k, 2, dx)
        inner_rows(k)
        collect(k)
        for dx in x_order:
            we_copy(k, dx).wait_send()
            n_copy(k, dx).wait_send()
            wi_copy(k, dx).wait_send()
        t_each(k, lambda copy: copy.wait_send())
        return carry

    lax.fori_loop(1, ITERS, iteration, 0)
    out[0] = ubuf[...]


def body(
    excitation,
    panel_points,
    panel_areas,
    panel_map,
    interior_inverse,
    row_scales,
    iface_slot,
    iface_offset,
    adjacency,
):
    strips = lax.axis_size("col")
    R = lax.axis_size("row")
    _, rhs, piece = excitation.shape
    block = strips * piece
    sub_width = interior_inverse.shape[3]
    X = sub_width // (GROUPS * piece)
    Z = strips // X
    Zh = Z // GROUPS
    RP = R * piece
    P_ = X * Zh
    vm = pltpu.VMEM
    dma = pltpu.SemaphoreType.DMA
    in_vmem = pl.BlockSpec(memory_space=pltpu.VMEM)
    return pl.pallas_call(
        functools.partial(kernel, (Z, X, R, piece, block)),
        out_shape=jax.ShapeDtypeStruct((1, rhs, piece), F32),
        in_specs=[in_vmem] * 6
        + [pl.BlockSpec(memory_space=pltpu.SMEM), pl.BlockSpec(memory_space=pl.ANY), in_vmem],
        out_specs=in_vmem,
        scratch_shapes=[
            vm((8, RP), F32),
            vm((8, piece), F32),
            vm((P_ * piece, 8), F32),
            vm((X, Zh, piece, RP), BF),
            vm((RP, X * piece), BF),
            vm((GROUPS * GROUPS, piece, X * piece), BF),
            vm((8, piece), jnp.int32),
            vm((Z, 8, piece), jnp.int32),
            vm((X, 8, piece), jnp.int32),
            vm((GROUPS, Z, rhs, piece), BF),
            vm((ITERS, rhs, piece), BF),
            vm((ITERS, GROUPS, Z, rhs, piece), BF),
            vm((ITERS, X, Zh, rhs, piece), BF),
            vm((ITERS, X, rhs, piece), BF),
            vm((ITERS, X, rhs, piece), BF),
            vm((ITERS, X, rhs, piece), BF),
            vm((rhs, RP), F32),
            vm((ITERS, GROUPS, R, rhs, piece), F32),
            vm((ITERS, GROUPS * R, rhs, piece), F32),
            vm((rhs, piece), F32),
            dma(()),
            dma((Z,)),
            dma((GROUPS, Z)),
            dma((Z,)),
            dma((Z,)),
            dma((GROUPS, Z)),
            dma((ITERS, GROUPS, Z)),
            dma((3, X)),
            dma((ITERS, 3, X)),
            dma((GROUPS, R)),
            dma((ITERS, GROUPS * R)),
        ],
        compiler_params=pltpu.CompilerParams(
            collective_id=0, has_side_effects=True, vmem_limit_bytes=60 * 1024 * 1024
        ),
    )(
        excitation,
        panel_points,
        panel_areas.reshape(1, -1),
        panel_map.reshape(1, -1),
        iface_slot.reshape(1, -1),
        iface_offset.reshape(1, -1),
        adjacency.T,
        interior_inverse[0, :, 0, :],
        row_scales,
    )


def solution(mesh):
    placed = (
        P("grp", None, ("row", "col")),
        P(),
        P(),
        P(("row", "col")),
        P("col", None, "row", None),
        P("col", None),
        P(("row", "col")),
        P(("row", "col")),
        P(),
    )
    return jax.shard_map(
        body, mesh=mesh, in_specs=placed, out_specs=P("grp", None, ("row", "col")), check_vma=False
    )
```

```python
import functools
import math

import jax
import jax.numpy as jnp
from jax import lax
from jax.experimental import pallas as pl
from jax.experimental.pallas import tpu as pltpu
from jax.sharding import PartitionSpec as P

ITERS = 4
GROUPS = 2
robin_weight = 0.5
iface_weight = 0.4
wave_number = 40.0
soften = 0.05
self_term = 0.5
KB = 32
X_CHIPS = 4

BF = jnp.bfloat16
F32 = jnp.float32
MESH = pl.DeviceIdType.MESH

COS_TERMS = (
    1.4142135381698608,
    -6.978850841522217,
    5.739460468292236,
    -1.883557915687561,
    0.3106880187988281,
)
TURNS = wave_number / (2.0 * math.pi)


def kernel(
    dims,
    exc,
    pts,
    areas,
    pmap,
    slot,
    off,
    adj,
    inv,
    scales,
    out,
    ipt,
    stage,
    kpt,
    kline,
    kbuf,
    abuf,
    gbuf,
    metasend,
    metabuf,
    xmeta,
    bbuf,
    tsend,
    tbuf,
    we,
    nsend,
    nbuf,
    wi,
    acc,
    psend,
    pbuf,
    ubuf,
    asem,
    b_s,
    b_r,
    m_s,
    m_r,
    t_s,
    t_r,
    x_s,
    x_r,
    y_s,
    y_r,
):
    Z, X, R, piece, block = dims
    Zh = Z // GROUPS
    sub_width = GROUPS * X * piece
    RP = R * piece
    g = lax.axis_index("grp")
    r = lax.axis_index("row")
    c = lax.axis_index("col")
    z, x = c // X, c % X
    s = z // GROUPS
    zt = GROUPS * s + g
    parity = z % GROUPS
    me = g * R + r

    def remote(src, dst, ss, rs, dev):
        return pltpu.make_async_remote_copy(
            src_ref=src, dst_ref=dst, send_sem=ss, recv_sem=rs, device_id=dev, device_id_type=MESH
        )

    def col_of(zz, xx):
        return zz * X + xx

    barrier = pltpu.get_barrier_semaphore()
    n_partners = 0
    for flip in range(GROUPS):
        for dz in range(Z):
            if flip or dz:
                pl.semaphore_signal(
                    barrier,
                    inc=1,
                    device_id={"grp": (g + flip) % GROUPS, "row": r, "col": col_of((z + dz) % Z, x)},
                    device_id_type=MESH,
                )
                n_partners += 1
    for dx in range(1, X):
        pl.semaphore_signal(
            barrier,
            inc=1,
            device_id={"grp": g, "row": r, "col": col_of(z, (x + dx) % X)},
            device_id_type=MESH,
        )
        n_partners += 1
    for flip in range(GROUPS):
        for dr in range(1, R):
            pl.semaphore_signal(
                barrier,
                inc=1,
                device_id={"grp": (g + flip) % GROUPS, "row": (r + dr) % R, "col": c},
                device_id_type=MESH,
            )
            n_partners += 1

    inverse_copy = pltpu.make_async_copy(
        inv.at[:, pl.ds(pl.multiple_of(g * X * piece, X * piece), X * piece)], abuf, asem
    )
    inverse_copy.start()

    for rr in range(R):
        start = pl.multiple_of(rr * block + c * piece, piece)
        own = pts[:, pl.ds(start, piece)] * TURNS
        for axis in range(3):
            ipt[axis, :, rr * piece : (rr + 1) * piece] = jnp.broadcast_to(
                own[axis : axis + 1, :], (KB, piece)
            )
    for p in range(X * Zh):
        xx, zi = p // Zh, p % Zh
        start = pl.multiple_of(r * block + col_of(GROUPS * zi + g, xx) * piece, piece)
        lanes = slice(p * piece, (p + 1) * piece)
        stage[0:3, lanes] = pts[:, pl.ds(start, piece)] * TURNS
        area = areas[:, pl.ds(start, piece)] * TURNS
        stage[3:4, lanes] = area
        root = jnp.sqrt(area)
        for n, term in enumerate(COS_TERMS):
            stage[4 + n : 5 + n, lanes] = root * term
        stage[9:16, lanes] = jnp.zeros((7, piece), F32)
    kpt[...] = jnp.transpose(stage[...])

    per_piece = piece // KB
    last_block = X * Zh * per_piece - 1
    LANES = 128
    PAIR = min(RP, 2 * LANES)

    def spread(t, to):
        kc = kpt[pl.ds(pl.multiple_of(t * KB, KB), KB), :]
        for n in range(9):
            kline[to, n] = jnp.broadcast_to(kc[:, n : n + 1], (KB, LANES))

    spread(0, 0)

    def make_rows(t, carry):
        p = t // per_piece
        row = pl.multiple_of((t % per_piece) * KB, KB)
        now = t % 2
        for m in range(RP // PAIR):
            halves = []
            for half in range(PAIR // LANES):
                first = m * PAIR + half * LANES
                lanes = slice(first, first + LANES)
                dx = ipt[0, :, lanes] - kline[now, 0]
                dy = ipt[1, :, lanes] - kline[now, 1]
                dz = ipt[2, :, lanes] - kline[now, 2]
                square = dx * dx + dy * dy + dz * dz
                turns = 1.0 / lax.rsqrt(square)
                part = turns - jnp.round(turns)
                v = part * part
                h = kline[now, 8] * v + kline[now, 7]
                h = h * v + kline[now, 6]
                h = h * v + kline[now, 5]
                h = h * v + kline[now, 4]
                top = h * h - kline[now, 3]
                halves.append(top / (turns + soften * TURNS))
            value = jnp.concatenate(halves, axis=1).astype(BF)
            kbuf[p // Zh, p % Zh, pl.ds(row, KB), m * PAIR : (m + 1) * PAIR] = value
        spread(jnp.minimum(t + 1, last_block), 1 - now)
        return carry

    quarter = X * Zh * per_piece // 4

    def make_quarter(q):
        lax.fori_loop(q * quarter, (q + 1) * quarter, make_rows, 0)

    make_quarter(0)
    pl.semaphore_wait(barrier, n_partners)

    metasend[...] = jnp.zeros_like(metasend)
    metasend[0:1, :] = pmap[...]
    metasend[1:2, :] = slot[...] * sub_width + off[...]
    b_plane = parity

    def b_copy(dz):
        return remote(
            exc.at[0],
            bbuf.at[g, z],
            b_s.at[dz],
            b_r.at[g, z],
            {"grp": b_plane, "row": r, "col": col_of((z + dz) % Z, x)},
        )

    def m_copy(dz):
        return remote(
            metasend,
            metabuf.at[z],
            m_s.at[dz],
            m_r.at[z],
            {"grp": g, "row": r, "col": col_of((z + dz) % Z, x)},
        )

    order = sorted(range(Z), key=lambda dz: -min(dz, Z - dz))
    for dz in order:
        if dz:
            b_copy(dz).start()

            @pl.when(b_plane == g)
            def _():
                m_copy(dz).start()
        else:

            @pl.when(b_plane != g)
            def _():
                b_copy(0).start()

            @pl.when(b_plane == g)
            def _():
                bbuf[g, z] = exc[0]
                metabuf[z] = metasend[...]

    make_quarter(1)

    for zi in range(Zh):
        zs = GROUPS * zi + g
        for src in range(GROUPS):

            @pl.when((zs != z) | (g != src))
            def _():
                remote(
                    bbuf.at[src, zs], bbuf.at[src, zs], b_s.at[0], b_r.at[src, zs], {"row": r}
                ).wait_recv()

        @pl.when(zs != z)
        def _():
            remote(metabuf.at[zs], metabuf.at[zs], m_s.at[0], m_r.at[zs], {"row": r}).wait_recv()

    def x_dev(dx):
        return {"grp": g, "row": r, "col": col_of(z, (x + dx) % X)}

    x_order = sorted(range(1, X), key=lambda dx: -min(dx, X - dx))

    def we_copy(k, dx):
        return remote(we.at[k, x], we.at[k, x], x_s.at[0, dx], x_r.at[k, 0, x], x_dev(dx))

    def n_copy(k, dx):
        return remote(
            nsend.at[k, (x + dx) % X], nbuf.at[k, x], x_s.at[1, dx], x_r.at[k, 1, x], x_dev(dx)
        )

    def wi_copy(k, dx):
        return remote(wi.at[k, x], wi.at[k, x], x_s.at[2, dx], x_r.at[k, 2, x], x_dev(dx))

    def xm_copy(dx):
        return remote(metabuf.at[zt], xmeta.at[x], x_s.at[1, dx], x_r.at[0, 1, x], x_dev(dx))

    def x_wait(ref, k, kind, dx):
        xs = (x + dx) % X
        remote(ref, ref, x_s.at[kind, dx], x_r.at[k, kind, xs], x_dev(dx)).wait_recv()

    for zi in range(Zh):
        we[0, x, zi] = bbuf[0, GROUPS * zi + g]
    wi[0, x] = bbuf[1, zt]
    xmeta[x] = metabuf[zt]
    for dx in x_order:
        we_copy(0, dx).start()
        xm_copy(dx).start()
        wi_copy(0, dx).start()
    make_quarter(2)

    for dx in range(1, X):
        xs = (x + dx) % X
        x_wait(xmeta.at[xs], 0, 1, dx)

    def make_gather(t, carry):
        xx, q = t // (GROUPS * GROUPS), t % (GROUPS * GROUPS)
        code = xmeta[xx, 1:2, :]
        src_x = (code // piece) % X
        src_q = code // (X * piece)
        here = jnp.where((src_x == x) & (src_q == q), code % piece, -1)
        rows = lax.broadcasted_iota(jnp.int32, (piece, piece), 0)
        hit = jnp.where(rows == here, 1.0, 0.0).astype(BF)
        gbuf[q, :, pl.ds(pl.multiple_of(xx * piece, piece), piece)] = hit
        return carry

    lax.fori_loop(0, X * GROUPS * GROUPS, make_gather, 0)
    make_quarter(3)
    inverse_copy.wait()
    for dx in range(1, X):
        x_wait(we.at[0, (x + dx) % X], 0, 0, dx)
        x_wait(wi.at[0, (x + dx) % X], 0, 2, dx)
        we_copy(0, dx).wait_send()
        xm_copy(dx).wait_send()
        wi_copy(0, dx).wait_send()
    for dz in order:
        if dz:
            b_copy(dz).wait_send()

            @pl.when(b_plane == g)
            def _():
                m_copy(dz).wait_send()
        else:

            @pl.when(b_plane != g)
            def _():
                b_copy(0).wait_send()

    def y_copy(k, kind, rr):
        return remote(
            psend.at[k, kind, rr],
            pbuf.at[k, me],
            y_s.at[kind, rr],
            y_r.at[k, me],
            {"grp": kind, "row": rr, "col": c},
        )

    def give(k, kind, rr, value):
        psend[k, kind, rr] = value
        own = (g == kind) & (r == rr)

        @pl.when(jnp.logical_not(own))
        def _():
            y_copy(k, kind, rr).start()

        @pl.when(own)
        def _():
            pbuf[k, me] = value

    def outer_part(k, xs, columns):
        total = None
        for zi in range(Zh):
            term = jnp.dot(we[k, xs, zi], kbuf[xs, zi, :, columns], preferred_element_type=F32)
            total = term if total is None else total + term
        return total

    everything = slice(None)

    def send_rows(k, xs):
        for j in range(R):
            rr = (r + 1 + j) % R
            columns = pl.ds(pl.multiple_of(rr * piece, piece), piece)
            value = acc[:, columns] + outer_part(k, xs, columns)
            own_piece = self_term * we[k, x, z // GROUPS].astype(F32)
            value = value + jnp.where((rr == r) & (parity == g), own_piece, 0.0)
            give(k, 0, rr, value)

    def inner_rows(k):
        for j in range(R):
            rr = (r + 1 + j) % R
            rows = pl.ds(pl.multiple_of(rr * piece, piece), piece)
            total = None
            for xx in range(X):
                term = lax.dot_general(
                    wi[k, xx],
                    abuf[rows, xx * piece : (xx + 1) * piece],
                    (((1,), (1,)), ((), ())),
                    preferred_element_type=F32,
                )
                total = term if total is None else total + term
            give(k, 1, rr, total)

    def collect(k):
        for src in range(GROUPS * R):

            @pl.when(src != me)
            def _():
                remote(
                    pbuf.at[k, src], pbuf.at[k, src], y_s.at[0, 0], y_r.at[k, src], {"row": r}
                ).wait_recv()

        total = pbuf[k, 0]
        for src in range(1, GROUPS * R):
            total = total + pbuf[k, src]
        scale = scales[:, pl.ds(pl.multiple_of(r * piece, piece), piece)]
        state = jnp.where(g == 0, total, scale * total)
        ubuf[...] = state
        tsend[k] = state.astype(BF)
        for kind in range(GROUPS):
            for rr in range(R):

                @pl.when((g != kind) | (r != rr))
                def _():
                    y_copy(k, kind, rr).wait_send()

    acc[...] = outer_part(0, 0, everything)
    for xx in range(1, X - 1):
        acc[...] += outer_part(0, xx, everything)
    send_rows(0, X - 1)
    inner_rows(0)
    collect(0)

    def t_copy(k, plane, dz):
        return remote(
            tsend.at[k - 1],
            tbuf.at[k, g, z],
            t_s.at[plane, dz],
            t_r.at[k, g, z],
            {"grp": plane, "row": r, "col": col_of((z + dz) % Z, x)},
        )

    def t_each(k, act):
        for dz in order:
            for plane in range(GROUPS):
                wanted = (g == 1) | (plane == parity)
                if dz == 0:
                    wanted = wanted & (plane != g)

                @pl.when(wanted)
                def _():
                    act(t_copy(k, plane, dz))

    def iteration(k, carry):
        t_each(k, lambda copy: copy.start())

        @pl.when((g == 1) | (parity == 0))
        def _():
            tbuf[k, g, z] = tsend[k - 1]

        for zz in range(Z):

            @pl.when((zz != z) | (g != 1))
            def _():
                remote(
                    tbuf.at[k, 1, zz], tbuf.at[k, 1, zz], t_s.at[0, 0], t_r.at[k, 1, zz], {"row": r}
                ).wait_recv()

        for zi in range(Zh):
            zs = GROUPS * zi + g

            @pl.when((zs != z) | (g != 0))
            def _():
                remote(
                    tbuf.at[k, 0, zs], tbuf.at[k, 0, zs], t_s.at[0, 0], t_r.at[k, 0, zs], {"row": r}
                ).wait_recv()

        near = None
        for j in range(GROUPS):
            for zz in range(GROUPS):
                source = tbuf[k, 1, zz].astype(F32)
                for n in range(1, Zh):
                    other = tbuf[k, 1, GROUPS * n + zz].astype(F32)
                    source = jnp.where(adj[j, s] == n, other, source)
                term = jnp.dot(
                    source.astype(BF), gbuf[j * GROUPS + zz], preferred_element_type=F32
                )
                near = term if near is None else near + term
        for xx in range(X):
            nsend[k, xx] = near[:, xx * piece : (xx + 1) * piece].astype(BF)
        for dx in x_order:
            n_copy(k, dx).start()

        for zi in range(Zh):
            zs = GROUPS * zi + g
            choice = metabuf[zs, 0:1, :]
            far = tbuf[k, 1, g].astype(F32)
            for n in range(1, Zh):
                far = jnp.where(choice == n, tbuf[k, 1, GROUPS * n + g].astype(F32), far)
            mixed = bbuf[0, zs].astype(F32) + robin_weight * (far - tbuf[k, 0, zs].astype(F32))
            we[k, x, zi] = mixed.astype(BF)
        for dx in x_order:
            we_copy(k, dx).start()

        acc[...] = outer_part(k, x, everything)

        near = nsend[k, x].astype(F32)
        for dx in range(1, X):
            xs = (x + dx) % X
            x_wait(nbuf.at[k, xs], k, 1, dx)
            near = near + nbuf[k, xs].astype(F32)
        inner = tbuf[k, 1, zt].astype(F32)
        outer = tbuf[k, 0, zt].astype(F32)
        mixed = (
            bbuf[1, zt].astype(F32)
            + robin_weight * (outer - inner)
            + iface_weight * (near - inner)
        )
        wi[k, x] = mixed.astype(BF)
        for dx in x_order:
            wi_copy(k, dx).start()

        x_near = x_order[::-1]
        for dx in x_near[:-1]:
            xs = (x + dx) % X
            x_wait(we.at[k, xs], k, 0, dx)
            acc[...] += outer_part(k, xs, everything)
        if X > 1:
            xs = (x + x_near[-1]) % X
            x_wait(we.at[k, xs], k, 0, x_near[-1])
        send_rows(k, xs if X > 1 else x)
        for dx in x_near:
            x_wait(wi.at[k, (x + dx) % X], k, 2, dx)
        inner_rows(k)
        collect(k)
        for dx in x_order:
            we_copy(k, dx).wait_send()
            n_copy(k, dx).wait_send()
            wi_copy(k, dx).wait_send()
        t_each(k, lambda copy: copy.wait_send())
        return carry

    lax.fori_loop(1, ITERS, iteration, 0)
    out[0] = ubuf[...]


def body(
    excitation,
    panel_points,
    panel_areas,
    panel_map,
    interior_inverse,
    row_scales,
    iface_slot,
    iface_offset,
    adjacency,
):
    strips = lax.axis_size("col")
    R = lax.axis_size("row")
    _, rhs, piece = excitation.shape
    block = strips * piece
    sub_width = interior_inverse.shape[3]
    X = sub_width // (GROUPS * piece)
    Z = strips // X
    Zh = Z // GROUPS
    RP = R * piece
    P_ = X * Zh
    vm = pltpu.VMEM
    dma = pltpu.SemaphoreType.DMA
    in_vmem = pl.BlockSpec(memory_space=pltpu.VMEM)
    return pl.pallas_call(
        functools.partial(kernel, (Z, X, R, piece, block)),
        out_shape=jax.ShapeDtypeStruct((1, rhs, piece), F32),
        in_specs=[in_vmem] * 6
        + [pl.BlockSpec(memory_space=pltpu.SMEM), pl.BlockSpec(memory_space=pl.ANY), in_vmem],
        out_specs=in_vmem,
        scratch_shapes=[
            vm((3, KB, RP), F32),
            vm((16, P_ * piece), F32),
            vm((P_ * piece, 16), F32),
            vm((2, 9, KB, 128), F32),
            vm((X, Zh, piece, RP), BF),
            vm((RP, X * piece), BF),
            vm((GROUPS * GROUPS, piece, X * piece), BF),
            vm((8, piece), jnp.int32),
            vm((Z, 8, piece), jnp.int32),
            vm((X, 8, piece), jnp.int32),
            vm((GROUPS, Z, rhs, piece), BF),
            vm((ITERS, rhs, piece), BF),
            vm((ITERS, GROUPS, Z, rhs, piece), BF),
            vm((ITERS, X, Zh, rhs, piece), BF),
            vm((ITERS, X, rhs, piece), BF),
            vm((ITERS, X, rhs, piece), BF),
            vm((ITERS, X, rhs, piece), BF),
            vm((rhs, RP), F32),
            vm((ITERS, GROUPS, R, rhs, piece), F32),
            vm((ITERS, GROUPS * R, rhs, piece), F32),
            vm((rhs, piece), F32),
            dma(()),
            dma((Z,)),
            dma((GROUPS, Z)),
            dma((Z,)),
            dma((Z,)),
            dma((GROUPS, Z)),
            dma((ITERS, GROUPS, Z)),
            dma((3, X)),
            dma((ITERS, 3, X)),
            dma((GROUPS, R)),
            dma((ITERS, GROUPS * R)),
        ],
        compiler_params=pltpu.CompilerParams(
            collective_id=0, has_side_effects=True, vmem_limit_bytes=60 * 1024 * 1024
        ),
    )(
        excitation,
        panel_points,
        panel_areas.reshape(1, -1),
        panel_map.reshape(1, -1),
        iface_slot.reshape(1, -1),
        iface_offset.reshape(1, -1),
        adjacency.T,
        interior_inverse[0, :, 0, :],
        row_scales,
    )


def solution(mesh):
    placed = (
        P("grp", None, ("row", "col")),
        P(),
        P(),
        P(("row", "col")),
        P("col", None, "row", None),
        P("col", None),
        P(("row", "col")),
        P(("row", "col")),
        P(),
    )
    return jax.shard_map(
        body, mesh=mesh, in_specs=placed, out_specs=P("grp", None, ("row", "col")), check_vma=False
    )
```

```python
import functools
import math

import jax
import jax.numpy as jnp
from jax import lax
from jax.experimental import pallas as pl
from jax.experimental.pallas import tpu as pltpu
from jax.sharding import PartitionSpec as P

ITERS = 4
GROUPS = 2
robin_weight = 0.5
iface_weight = 0.4
wave_number = 40.0
soften = 0.05
self_term = 0.5
KB = 32
X_CHIPS = 4

BF = jnp.bfloat16
F32 = jnp.float32
MESH = pl.DeviceIdType.MESH

COS_TERMS = (
    1.4142135381698608,
    -6.978850841522217,
    5.739460468292236,
    -1.883557915687561,
    0.3106880187988281,
)
TURNS = wave_number / (2.0 * math.pi)


def kernel(
    dims,
    exc,
    pts,
    areas,
    pmap,
    slot,
    off,
    adj,
    inv,
    scales,
    out,
    ipt,
    stage,
    kpt,
    kline,
    kbuf,
    abuf,
    gbuf,
    metasend,
    metabuf,
    xmeta,
    bbuf,
    tsend,
    tbuf,
    we,
    nsend,
    nbuf,
    wi,
    acc,
    psend,
    pbuf,
    ubuf,
    asem,
    b_s,
    b_r,
    m_s,
    m_r,
    t_s,
    t_r,
    x_s,
    x_r,
    y_s,
    y_r,
):
    Z, X, R, piece, block = dims
    Zh = Z // GROUPS
    sub_width = GROUPS * X * piece
    RP = R * piece
    g = lax.axis_index("grp")
    r = lax.axis_index("row")
    c = lax.axis_index("col")
    z, x = c // X, c % X
    s = z // GROUPS
    zt = GROUPS * s + g
    parity = z % GROUPS
    me = g * R + r

    def remote(src, dst, ss, rs, dev):
        return pltpu.make_async_remote_copy(
            src_ref=src, dst_ref=dst, send_sem=ss, recv_sem=rs, device_id=dev, device_id_type=MESH
        )

    def col_of(zz, xx):
        return zz * X + xx

    barrier = pltpu.get_barrier_semaphore()
    n_partners = 0
    for flip in range(GROUPS):
        for dz in range(Z):
            if flip or dz:
                pl.semaphore_signal(
                    barrier,
                    inc=1,
                    device_id={"grp": (g + flip) % GROUPS, "row": r, "col": col_of((z + dz) % Z, x)},
                    device_id_type=MESH,
                )
                n_partners += 1
    for dx in range(1, X):
        pl.semaphore_signal(
            barrier,
            inc=1,
            device_id={"grp": g, "row": r, "col": col_of(z, (x + dx) % X)},
            device_id_type=MESH,
        )
        n_partners += 1
    for flip in range(GROUPS):
        for dr in range(1, R):
            pl.semaphore_signal(
                barrier,
                inc=1,
                device_id={"grp": (g + flip) % GROUPS, "row": (r + dr) % R, "col": c},
                device_id_type=MESH,
            )
            n_partners += 1

    inverse_copy = pltpu.make_async_copy(
        inv.at[:, pl.ds(pl.multiple_of(g * X * piece, X * piece), X * piece)], abuf, asem
    )
    inverse_copy.start()

    for rr in range(R):
        start = pl.multiple_of(rr * block + c * piece, piece)
        own = pts[:, pl.ds(start, piece)] * TURNS
        for axis in range(3):
            ipt[axis, :, rr * piece : (rr + 1) * piece] = jnp.broadcast_to(
                own[axis : axis + 1, :], (KB, piece)
            )
    for p in range(X * Zh):
        xx, zi = p // Zh, p % Zh
        start = pl.multiple_of(r * block + col_of(GROUPS * zi + g, xx) * piece, piece)
        lanes = slice(p * piece, (p + 1) * piece)
        stage[0:3, lanes] = pts[:, pl.ds(start, piece)] * TURNS
        area = areas[:, pl.ds(start, piece)] * TURNS
        stage[3:4, lanes] = area
        root = jnp.sqrt(area)
        for n, term in enumerate(COS_TERMS):
            stage[4 + n : 5 + n, lanes] = root * term
        stage[9:16, lanes] = jnp.zeros((7, piece), F32)
    kpt[...] = jnp.transpose(stage[...])

    per_piece = piece // KB
    last_block = X * Zh * per_piece - 1
    LANES = 128
    PAIR = min(RP, 2 * LANES)

    def spread(t, to):
        kc = kpt[pl.ds(pl.multiple_of(t * KB, KB), KB), :]
        for n in range(9):
            kline[to, n] = jnp.broadcast_to(kc[:, n : n + 1], (KB, LANES))

    spread(0, 0)

    def make_rows(t, carry):
        p = t // per_piece
        row = pl.multiple_of((t % per_piece) * KB, KB)
        now = t % 2
        for m in range(RP // PAIR):
            halves = []
            for half in range(PAIR // LANES):
                first = m * PAIR + half * LANES
                lanes = slice(first, first + LANES)
                dx = ipt[0, :, lanes] - kline[now, 0]
                dy = ipt[1, :, lanes] - kline[now, 1]
                dz = ipt[2, :, lanes] - kline[now, 2]
                square = dx * dx + dy * dy + dz * dz
                turns = 1.0 / lax.rsqrt(square)
                part = turns - jnp.round(turns)
                v = part * part
                h = kline[now, 8] * v + kline[now, 7]
                h = h * v + kline[now, 6]
                h = h * v + kline[now, 5]
                h = h * v + kline[now, 4]
                top = h * h - kline[now, 3]
                halves.append(top / (turns + soften * TURNS))
            value = jnp.concatenate(halves, axis=1).astype(BF)
            kbuf[p // Zh, p % Zh, pl.ds(row, KB), m * PAIR : (m + 1) * PAIR] = value
        spread(jnp.minimum(t + 1, last_block), 1 - now)
        return carry

    trips = X * Zh * per_piece
    cuts = (0, trips * 7 // 16, trips * 12 // 16, trips)

    def make_part(q):
        lax.fori_loop(cuts[q], cuts[q + 1], make_rows, 0)

    make_part(0)
    pl.semaphore_wait(barrier, n_partners)

    metasend[...] = jnp.zeros_like(metasend)
    metasend[0:1, :] = pmap[...]
    metasend[1:2, :] = slot[...] * sub_width + off[...]
    b_plane = parity

    def b_copy(dz):
        return remote(
            exc.at[0],
            bbuf.at[g, z],
            b_s.at[dz],
            b_r.at[g, z],
            {"grp": b_plane, "row": r, "col": col_of((z + dz) % Z, x)},
        )

    def m_copy(dz):
        return remote(
            metasend,
            metabuf.at[z],
            m_s.at[dz],
            m_r.at[z],
            {"grp": g, "row": r, "col": col_of((z + dz) % Z, x)},
        )

    order = sorted(range(Z), key=lambda dz: -min(dz, Z - dz))
    for dz in order:
        if dz:
            b_copy(dz).start()

            @pl.when(b_plane == g)
            def _():
                m_copy(dz).start()
        else:

            @pl.when(b_plane != g)
            def _():
                b_copy(0).start()

            @pl.when(b_plane == g)
            def _():
                bbuf[g, z] = exc[0]
                metabuf[z] = metasend[...]

    make_part(1)

    for zi in range(Zh):
        zs = GROUPS * zi + g
        for src in range(GROUPS):

            @pl.when((zs != z) | (g != src))
            def _():
                remote(
                    bbuf.at[src, zs], bbuf.at[src, zs], b_s.at[0], b_r.at[src, zs], {"row": r}
                ).wait_recv()

        @pl.when(zs != z)
        def _():
            remote(metabuf.at[zs], metabuf.at[zs], m_s.at[0], m_r.at[zs], {"row": r}).wait_recv()

    def x_dev(dx):
        return {"grp": g, "row": r, "col": col_of(z, (x + dx) % X)}

    x_order = sorted(range(1, X), key=lambda dx: -min(dx, X - dx))

    def we_copy(k, dx):
        return remote(we.at[k, x], we.at[k, x], x_s.at[0, dx], x_r.at[k, 0, x], x_dev(dx))

    def n_copy(k, dx):
        return remote(
            nsend.at[k, (x + dx) % X], nbuf.at[k, x], x_s.at[1, dx], x_r.at[k, 1, x], x_dev(dx)
        )

    def wi_copy(k, dx):
        return remote(wi.at[k, x], wi.at[k, x], x_s.at[2, dx], x_r.at[k, 2, x], x_dev(dx))

    def xm_copy(dx):
        return remote(metabuf.at[zt], xmeta.at[x], x_s.at[1, dx], x_r.at[0, 1, x], x_dev(dx))

    def x_wait(ref, k, kind, dx):
        xs = (x + dx) % X
        remote(ref, ref, x_s.at[kind, dx], x_r.at[k, kind, xs], x_dev(dx)).wait_recv()

    for zi in range(Zh):
        we[0, x, zi] = bbuf[0, GROUPS * zi + g]
    wi[0, x] = bbuf[1, zt]
    xmeta[x] = metabuf[zt]
    for dx in x_order:
        we_copy(0, dx).start()
        xm_copy(dx).start()
        wi_copy(0, dx).start()
    make_part(2)

    def make_gather(t, carry):
        xx, q = t // (GROUPS * GROUPS), t % (GROUPS * GROUPS)
        code = xmeta[xx, 1:2, :]
        src_x = (code // piece) % X
        src_q = code // (X * piece)
        here = jnp.where((src_x == x) & (src_q == q), code % piece, -1)
        rows = lax.broadcasted_iota(jnp.int32, (piece, piece), 0)
        hit = jnp.where(rows == here, 1.0, 0.0).astype(BF)
        gbuf[q, :, pl.ds(pl.multiple_of(xx * piece, piece), piece)] = hit
        return carry

    inverse_copy.wait()
    for dx in range(1, X):
        x_wait(we.at[0, (x + dx) % X], 0, 0, dx)
        x_wait(wi.at[0, (x + dx) % X], 0, 2, dx)
        x_wait(xmeta.at[(x + dx) % X], 0, 1, dx)
        we_copy(0, dx).wait_send()
        xm_copy(dx).wait_send()
        wi_copy(0, dx).wait_send()
    for dz in order:
        if dz:
            b_copy(dz).wait_send()

            @pl.when(b_plane == g)
            def _():
                m_copy(dz).wait_send()
        else:

            @pl.when(b_plane != g)
            def _():
                b_copy(0).wait_send()

    def is_last(k):
        return jnp.int32(k) == ITERS - 1

    def y_plane(k, way):
        return jnp.where(is_last(k), 0, parity) if way == 0 else 2 - way

    def y_copy(k, way, rr):
        kind = min(way, 1)
        return remote(
            psend.at[k, kind, rr],
            pbuf.at[k, kind, me],
            y_s.at[way, rr],
            y_r.at[k, kind, me],
            {"grp": y_plane(k, way), "row": rr, "col": c},
        )

    def y_other(k, way, rr):
        other = (g != y_plane(k, way)) | (r != rr)
        return other & jnp.logical_not(is_last(k)) if way == 2 else other

    def give(k, kind, rr, value):
        psend[k, kind, rr] = value
        for way in ((0,), (1, 2))[kind]:

            @pl.when(y_other(k, way, rr))
            def _():
                y_copy(k, way, rr).start()

    def t_copy(k, kind, dz):
        return remote(
            tsend.at[k, kind],
            tbuf.at[k + 1, kind, z],
            t_s.at[kind, dz],
            t_r.at[k + 1, kind, z],
            {"grp": g, "row": r, "col": col_of((z + dz) % Z, x)},
        )

    def outer_part(k, xs, columns):
        total = None
        for zi in range(Zh):
            term = jnp.dot(we[k, xs, zi], kbuf[xs, zi, :, columns], preferred_element_type=F32)
            total = term if total is None else total + term
        return total

    everything = slice(None)

    def send_rows(k, xs):
        for j in range(R):
            rr = (r + 1 + j) % R
            columns = pl.ds(pl.multiple_of(rr * piece, piece), piece)
            value = acc[:, columns] + outer_part(k, xs, columns)
            own_piece = self_term * we[k, x, z // GROUPS].astype(F32)
            value = value + jnp.where((rr == r) & (parity == g), own_piece, 0.0)
            give(k, 0, rr, value)

    def inner_rows(k):
        for j in range(R):
            rr = (r + 1 + j) % R
            rows = pl.ds(pl.multiple_of(rr * piece, piece), piece)
            total = None
            for xx in range(X):
                term = lax.dot_general(
                    wi[k, xx],
                    abuf[rows, xx * piece : (xx + 1) * piece],
                    (((1,), (1,)), ((), ())),
                    preferred_element_type=F32,
                )
                total = term if total is None else total + term
            give(k, 1, rr, total)

    def collect(k):
        for kind in range(GROUPS):
            takes = (
                jnp.where(is_last(k), 0, parity) == g
                if kind == 0
                else jnp.logical_not(is_last(k)) | (g == 1)
            )
            for src in range(GROUPS * R):

                @pl.when(takes & (src != me))
                def _():
                    remote(
                        pbuf.at[k, kind, src],
                        pbuf.at[k, kind, src],
                        y_s.at[0, 0],
                        y_r.at[k, kind, src],
                        {"row": r},
                    ).wait_recv()

            @pl.when(takes)
            def _():
                pbuf[k, kind, me] = psend[k, kind, r]
                total = pbuf[k, kind, 0]
                for src in range(1, GROUPS * R):
                    total = total + pbuf[k, kind, src]
                if kind == 1:
                    total = total * scales[:, pl.ds(pl.multiple_of(r * piece, piece), piece)]

                @pl.when(is_last(k))
                def _():
                    ubuf[...] = total

                @pl.when(jnp.logical_not(is_last(k)))
                def _():
                    trace = total.astype(BF)
                    tsend[k, kind] = trace
                    for dz in order:
                        if dz:
                            t_copy(k, kind, dz).start()
                    tbuf[k + 1, kind, z] = trace

        for way in range(3):
            for rr in range(R):

                @pl.when(y_other(k, way, rr))
                def _():
                    y_copy(k, way, rr).wait_send()

    def t_sent(k):
        for kind in range(GROUPS):

            @pl.when((kind == 1) | (parity == g))
            def _():
                for dz in order:
                    if dz:
                        t_copy(k, kind, dz).wait_send()

    acc[...] = outer_part(0, 0, everything)
    for xx in range(1, X - 1):
        acc[...] += outer_part(0, xx, everything)
    send_rows(0, X - 1)
    inner_rows(0)
    lax.fori_loop(0, X * GROUPS * GROUPS, make_gather, 0)
    collect(0)

    def iteration(k, carry):
        for zz in range(Z):

            @pl.when(zz != z)
            def _():
                remote(
                    tbuf.at[k, 1, zz], tbuf.at[k, 1, zz], t_s.at[0, 0], t_r.at[k, 1, zz], {"row": r}
                ).wait_recv()

        for zi in range(Zh):
            zs = GROUPS * zi + g

            @pl.when(zs != z)
            def _():
                remote(
                    tbuf.at[k, 0, zs], tbuf.at[k, 0, zs], t_s.at[0, 0], t_r.at[k, 0, zs], {"row": r}
                ).wait_recv()

        near = None
        for j in range(GROUPS):
            for zz in range(GROUPS):
                source = tbuf[k, 1, zz].astype(F32)
                for n in range(1, Zh):
                    other = tbuf[k, 1, GROUPS * n + zz].astype(F32)
                    source = jnp.where(adj[j, s] == n, other, source)
                term = jnp.dot(
                    source.astype(BF), gbuf[j * GROUPS + zz], preferred_element_type=F32
                )
                near = term if near is None else near + term
        for xx in range(X):
            nsend[k, xx] = near[:, xx * piece : (xx + 1) * piece].astype(BF)
        for dx in x_order:
            n_copy(k, dx).start()

        for zi in range(Zh):
            zs = GROUPS * zi + g
            choice = metabuf[zs, 0:1, :]
            far = tbuf[k, 1, g].astype(F32)
            for n in range(1, Zh):
                far = jnp.where(choice == n, tbuf[k, 1, GROUPS * n + g].astype(F32), far)
            mixed = bbuf[0, zs].astype(F32) + robin_weight * (far - tbuf[k, 0, zs].astype(F32))
            we[k, x, zi] = mixed.astype(BF)
        for dx in x_order:
            we_copy(k, dx).start()

        acc[...] = outer_part(k, x, everything)

        near = nsend[k, x].astype(F32)
        for dx in range(1, X):
            xs = (x + dx) % X
            x_wait(nbuf.at[k, xs], k, 1, dx)
            near = near + nbuf[k, xs].astype(F32)
        inner = tbuf[k, 1, zt].astype(F32)
        outer = tbuf[k, 0, zt].astype(F32)
        mixed = (
            bbuf[1, zt].astype(F32)
            + robin_weight * (outer - inner)
            + iface_weight * (near - inner)
        )
        wi[k, x] = mixed.astype(BF)
        for dx in x_order:
            wi_copy(k, dx).start()

        x_near = x_order[::-1]
        for dx in x_near[:-1]:
            xs = (x + dx) % X
            x_wait(we.at[k, xs], k, 0, dx)
            acc[...] += outer_part(k, xs, everything)
        if X > 1:
            xs = (x + x_near[-1]) % X
            x_wait(we.at[k, xs], k, 0, x_near[-1])
        send_rows(k, xs if X > 1 else x)
        for dx in x_near:
            x_wait(wi.at[k, (x + dx) % X], k, 2, dx)
        inner_rows(k)
        t_sent(k - 1)
        collect(k)
        for dx in x_order:
            we_copy(k, dx).wait_send()
            n_copy(k, dx).wait_send()
            wi_copy(k, dx).wait_send()
        return carry

    lax.fori_loop(1, ITERS, iteration, 0)
    out[0] = ubuf[...]


def body(
    excitation,
    panel_points,
    panel_areas,
    panel_map,
    interior_inverse,
    row_scales,
    iface_slot,
    iface_offset,
    adjacency,
):
    strips = lax.axis_size("col")
    R = lax.axis_size("row")
    _, rhs, piece = excitation.shape
    block = strips * piece
    sub_width = interior_inverse.shape[3]
    X = sub_width // (GROUPS * piece)
    Z = strips // X
    Zh = Z // GROUPS
    RP = R * piece
    P_ = X * Zh
    vm = pltpu.VMEM
    dma = pltpu.SemaphoreType.DMA
    in_vmem = pl.BlockSpec(memory_space=pltpu.VMEM)
    return pl.pallas_call(
        functools.partial(kernel, (Z, X, R, piece, block)),
        out_shape=jax.ShapeDtypeStruct((1, rhs, piece), F32),
        in_specs=[in_vmem] * 6
        + [pl.BlockSpec(memory_space=pltpu.SMEM), pl.BlockSpec(memory_space=pl.ANY), in_vmem],
        out_specs=in_vmem,
        scratch_shapes=[
            vm((3, KB, RP), F32),
            vm((16, P_ * piece), F32),
            vm((P_ * piece, 16), F32),
            vm((2, 9, KB, 128), F32),
            vm((X, Zh, piece, RP), BF),
            vm((RP, X * piece), BF),
            vm((GROUPS * GROUPS, piece, X * piece), BF),
            vm((8, piece), jnp.int32),
            vm((Z, 8, piece), jnp.int32),
            vm((X, 8, piece), jnp.int32),
            vm((GROUPS, Z, rhs, piece), BF),
            vm((ITERS, GROUPS, rhs, piece), BF),
            vm((ITERS, GROUPS, Z, rhs, piece), BF),
            vm((ITERS, X, Zh, rhs, piece), BF),
            vm((ITERS, X, rhs, piece), BF),
            vm((ITERS, X, rhs, piece), BF),
            vm((ITERS, X, rhs, piece), BF),
            vm((rhs, RP), F32),
            vm((ITERS, GROUPS, R, rhs, piece), F32),
            vm((ITERS, GROUPS, GROUPS * R, rhs, piece), F32),
            vm((rhs, piece), F32),
            dma(()),
            dma((Z,)),
            dma((GROUPS, Z)),
            dma((Z,)),
            dma((Z,)),
            dma((GROUPS, Z)),
            dma((ITERS, GROUPS, Z)),
            dma((3, X)),
            dma((ITERS, 3, X)),
            dma((3, R)),
            dma((ITERS, GROUPS, GROUPS * R)),
        ],
        compiler_params=pltpu.CompilerParams(
            collective_id=0, has_side_effects=True, vmem_limit_bytes=60 * 1024 * 1024
        ),
    )(
        excitation,
        panel_points,
        panel_areas.reshape(1, -1),
        panel_map.reshape(1, -1),
        iface_slot.reshape(1, -1),
        iface_offset.reshape(1, -1),
        adjacency.T,
        interior_inverse[0, :, 0, :],
        row_scales,
    )


def solution(mesh):
    placed = (
        P("grp", None, ("row", "col")),
        P(),
        P(),
        P(("row", "col")),
        P("col", None, "row", None),
        P("col", None),
        P(("row", "col")),
        P(("row", "col")),
        P(),
    )
    return jax.shard_map(
        body, mesh=mesh, in_specs=placed, out_specs=P("grp", None, ("row", "col")), check_vma=False
    )
```

```python
import functools
import math

import jax
import jax.numpy as jnp
from jax import lax
from jax.experimental import pallas as pl
from jax.experimental.pallas import tpu as pltpu
from jax.sharding import PartitionSpec as P

ITERS = 4
GROUPS = 2
robin_weight = 0.5
iface_weight = 0.4
wave_number = 40.0
soften = 0.05
self_term = 0.5
KB = 32
X_CHIPS = 4

BF = jnp.bfloat16
F32 = jnp.float32
MESH = pl.DeviceIdType.MESH

COS_TERMS = (
    1.4142135381698608,
    -6.978850841522217,
    5.739460468292236,
    -1.883557915687561,
    0.3106880187988281,
)
TURNS = wave_number / (2.0 * math.pi)


def kernel(
    dims,
    exc,
    pts,
    areas,
    pmap,
    slot,
    off,
    adj,
    inv,
    scales,
    out,
    ipt,
    stage,
    kpt,
    kline,
    kbuf,
    abuf,
    gbuf,
    metasend,
    metabuf,
    xmeta,
    bbuf,
    tsend,
    tbuf,
    we,
    nsend,
    nbuf,
    wi,
    acc,
    inner,
    psend,
    pbuf,
    ubuf,
    asem,
    b_s,
    b_r,
    m_s,
    m_r,
    t_s,
    t_r,
    x_s,
    x_r,
    y_s,
    y_r,
):
    Z, X, R, piece, block = dims
    Zh = Z // GROUPS
    sub_width = GROUPS * X * piece
    RP = R * piece
    g = lax.axis_index("grp")
    r = lax.axis_index("row")
    c = lax.axis_index("col")
    z, x = c // X, c % X
    s = z // GROUPS
    zt = GROUPS * s + g
    parity = z % GROUPS
    me = g * R + r

    def remote(src, dst, ss, rs, dev):
        return pltpu.make_async_remote_copy(
            src_ref=src, dst_ref=dst, send_sem=ss, recv_sem=rs, device_id=dev, device_id_type=MESH
        )

    def col_of(zz, xx):
        return zz * X + xx

    barrier = pltpu.get_barrier_semaphore()
    n_partners = 0
    for flip in range(GROUPS):
        for dz in range(Z):
            if flip or dz:
                pl.semaphore_signal(
                    barrier,
                    inc=1,
                    device_id={"grp": (g + flip) % GROUPS, "row": r, "col": col_of((z + dz) % Z, x)},
                    device_id_type=MESH,
                )
                n_partners += 1
    for dx in range(1, X):
        pl.semaphore_signal(
            barrier,
            inc=1,
            device_id={"grp": g, "row": r, "col": col_of(z, (x + dx) % X)},
            device_id_type=MESH,
        )
        n_partners += 1
    for flip in range(GROUPS):
        for dr in range(1, R):
            pl.semaphore_signal(
                barrier,
                inc=1,
                device_id={"grp": (g + flip) % GROUPS, "row": (r + dr) % R, "col": c},
                device_id_type=MESH,
            )
            n_partners += 1

    inverse_copy = pltpu.make_async_copy(
        inv.at[:, pl.ds(pl.multiple_of(g * X * piece, X * piece), X * piece)], abuf, asem
    )
    inverse_copy.start()

    for rr in range(R):
        start = pl.multiple_of(rr * block + c * piece, piece)
        own = pts[:, pl.ds(start, piece)] * TURNS
        for axis in range(3):
            ipt[axis, :, rr * piece : (rr + 1) * piece] = jnp.broadcast_to(
                own[axis : axis + 1, :], (KB, piece)
            )
    for p in range(X * Zh):
        xx, zi = p // Zh, p % Zh
        start = pl.multiple_of(r * block + col_of(GROUPS * zi + g, xx) * piece, piece)
        lanes = slice(p * piece, (p + 1) * piece)
        stage[0:3, lanes] = pts[:, pl.ds(start, piece)] * TURNS
        area = areas[:, pl.ds(start, piece)] * TURNS
        stage[3:4, lanes] = area
        root = jnp.sqrt(area)
        for n, term in enumerate(COS_TERMS):
            stage[4 + n : 5 + n, lanes] = root * term
        stage[9:16, lanes] = jnp.zeros((7, piece), F32)
    kpt[...] = jnp.transpose(stage[...])

    per_piece = piece // KB
    last_block = X * Zh * per_piece - 1
    LANES = 128
    PAIR = min(RP, 2 * LANES)

    def spread(t, to):
        kc = kpt[pl.ds(pl.multiple_of(t * KB, KB), KB), :]
        for n in range(9):
            kline[to, n] = jnp.broadcast_to(kc[:, n : n + 1], (KB, LANES))

    spread(0, 0)

    def make_rows(t, carry):
        p = t // per_piece
        row = pl.multiple_of((t % per_piece) * KB, KB)
        now = t % 2
        for m in range(RP // PAIR):
            halves = []
            for half in range(PAIR // LANES):
                first = m * PAIR + half * LANES
                lanes = slice(first, first + LANES)
                dx = ipt[0, :, lanes] - kline[now, 0]
                dy = ipt[1, :, lanes] - kline[now, 1]
                dz = ipt[2, :, lanes] - kline[now, 2]
                square = dx * dx + dy * dy + dz * dz
                turns = 1.0 / lax.rsqrt(square)
                part = turns - jnp.round(turns)
                v = part * part
                h = kline[now, 8] * v + kline[now, 7]
                h = h * v + kline[now, 6]
                h = h * v + kline[now, 5]
                h = h * v + kline[now, 4]
                top = h * h - kline[now, 3]
                halves.append(top / (turns + soften * TURNS))
            value = jnp.concatenate(halves, axis=1).astype(BF)
            kbuf[p // Zh, p % Zh, pl.ds(row, KB), m * PAIR : (m + 1) * PAIR] = value
        spread(jnp.minimum(t + 1, last_block), 1 - now)
        return carry

    trips = X * Zh * per_piece
    cuts = (0, trips * 7 // 16, trips * 12 // 16, trips)

    def make_part(q):
        lax.fori_loop(cuts[q], cuts[q + 1], make_rows, 0)

    make_part(0)
    pl.semaphore_wait(barrier, n_partners)

    metasend[...] = jnp.zeros_like(metasend)
    metasend[0:1, :] = pmap[...]
    metasend[1:2, :] = slot[...] * sub_width + off[...]
    b_plane = parity

    def b_copy(dz):
        return remote(
            exc.at[0],
            bbuf.at[g, z],
            b_s.at[dz],
            b_r.at[g, z],
            {"grp": b_plane, "row": r, "col": col_of((z + dz) % Z, x)},
        )

    def m_copy(dz):
        return remote(
            metasend,
            metabuf.at[z],
            m_s.at[dz],
            m_r.at[z],
            {"grp": g, "row": r, "col": col_of((z + dz) % Z, x)},
        )

    order = sorted(range(Z), key=lambda dz: -min(dz, Z - dz))
    for dz in order:
        if dz:
            b_copy(dz).start()

            @pl.when(b_plane == g)
            def _():
                m_copy(dz).start()
        else:

            @pl.when(b_plane != g)
            def _():
                b_copy(0).start()

            @pl.when(b_plane == g)
            def _():
                bbuf[g, z] = exc[0]
                metabuf[z] = metasend[...]

    make_part(1)

    for zi in range(Zh):
        zs = GROUPS * zi + g
        for src in range(GROUPS):

            @pl.when((zs != z) | (g != src))
            def _():
                remote(
                    bbuf.at[src, zs], bbuf.at[src, zs], b_s.at[0], b_r.at[src, zs], {"row": r}
                ).wait_recv()

        @pl.when(zs != z)
        def _():
            remote(metabuf.at[zs], metabuf.at[zs], m_s.at[0], m_r.at[zs], {"row": r}).wait_recv()

    def x_dev(dx):
        return {"grp": g, "row": r, "col": col_of(z, (x + dx) % X)}

    x_order = sorted(range(1, X), key=lambda dx: -min(dx, X - dx))

    def we_copy(k, dx):
        return remote(we.at[k, x], we.at[k, x], x_s.at[0, dx], x_r.at[k, 0, x], x_dev(dx))

    def n_copy(k, dx):
        return remote(
            nsend.at[k, (x + dx) % X], nbuf.at[k, x], x_s.at[1, dx], x_r.at[k, 1, x], x_dev(dx)
        )

    def wi_copy(k, dx):
        return remote(wi.at[k, x], wi.at[k, x], x_s.at[2, dx], x_r.at[k, 2, x], x_dev(dx))

    def xm_copy(dx):
        return remote(metabuf.at[zt], xmeta.at[x], x_s.at[1, dx], x_r.at[0, 1, x], x_dev(dx))

    def x_wait(ref, k, kind, dx):
        xs = (x + dx) % X
        remote(ref, ref, x_s.at[kind, dx], x_r.at[k, kind, xs], x_dev(dx)).wait_recv()

    for zi in range(Zh):
        we[0, x, zi] = bbuf[0, GROUPS * zi + g]
    wi[0, x] = bbuf[1, zt]
    xmeta[x] = metabuf[zt]
    for dx in x_order:
        we_copy(0, dx).start()
        xm_copy(dx).start()
        wi_copy(0, dx).start()
    make_part(2)

    def make_gather(t, carry):
        xx, q = t // (GROUPS * GROUPS), t % (GROUPS * GROUPS)
        code = xmeta[xx, 1:2, :]
        src_x = (code // piece) % X
        src_q = code // (X * piece)
        here = jnp.where((src_x == x) & (src_q == q), code % piece, -1)
        rows = lax.broadcasted_iota(jnp.int32, (piece, piece), 0)
        hit = jnp.where(rows == here, 1.0, 0.0).astype(BF)
        gbuf[q, :, pl.ds(pl.multiple_of(xx * piece, piece), piece)] = hit
        return carry

    inverse_copy.wait()
    for dx in range(1, X):
        x_wait(we.at[0, (x + dx) % X], 0, 0, dx)
        x_wait(wi.at[0, (x + dx) % X], 0, 2, dx)
        x_wait(xmeta.at[(x + dx) % X], 0, 1, dx)
        we_copy(0, dx).wait_send()
        xm_copy(dx).wait_send()
        wi_copy(0, dx).wait_send()
    for dz in order:
        if dz:
            b_copy(dz).wait_send()

            @pl.when(b_plane == g)
            def _():
                m_copy(dz).wait_send()
        else:

            @pl.when(b_plane != g)
            def _():
                b_copy(0).wait_send()

    def is_last(k):
        return jnp.int32(k) == ITERS - 1

    def y_plane(k, way):
        return jnp.where(is_last(k), 0, parity) if way == 0 else 2 - way

    def y_copy(k, way, rr):
        kind = min(way, 1)
        return remote(
            psend.at[k, kind, rr],
            pbuf.at[k, kind, me],
            y_s.at[way, rr],
            y_r.at[k, kind, me],
            {"grp": y_plane(k, way), "row": rr, "col": c},
        )

    def y_other(k, way, rr):
        other = (g != y_plane(k, way)) | (r != rr)
        return other & jnp.logical_not(is_last(k)) if way == 2 else other

    def give(k, kind, rr, value):
        psend[k, kind, rr] = value
        for way in ((0,), (1, 2))[kind]:

            @pl.when(y_other(k, way, rr))
            def _():
                y_copy(k, way, rr).start()

    def t_copy(k, kind, dz):
        return remote(
            tsend.at[k, kind],
            tbuf.at[k + 1, kind, z],
            t_s.at[kind, dz],
            t_r.at[k + 1, kind, z],
            {"grp": g, "row": r, "col": col_of((z + dz) % Z, x)},
        )

    def outer_part(k, xs, columns):
        total = None
        for zi in range(Zh):
            term = jnp.dot(we[k, xs, zi], kbuf[xs, zi, :, columns], preferred_element_type=F32)
            total = term if total is None else total + term
        return total

    everything = slice(None)
    cores = min(R, 2)
    row_order = []
    for far in reversed(range(R // cores)):
        for side in reversed(range(cores)):
            row_order.append(
                ((r // cores + far) % (R // cores)) * cores + (r % cores + side) % cores
            )

    def send_rows(k, xs):
        for rr in row_order:
            columns = pl.ds(pl.multiple_of(rr * piece, piece), piece)
            value = acc[:, columns] + outer_part(k, xs, columns)
            own_piece = self_term * we[k, x, z // GROUPS].astype(F32)
            value = value + jnp.where((rr == r) & (parity == g), own_piece, 0.0)
            give(k, 0, rr, value)

    def inner_part(k, xs, rows):
        return lax.dot_general(
            wi[k, xs],
            abuf[rows, pl.ds(pl.multiple_of(xs * piece, piece), piece)],
            (((1,), (1,)), ((), ())),
            preferred_element_type=F32,
        )

    def inner_rows(k, xs):
        for rr in row_order:
            rows = pl.ds(pl.multiple_of(rr * piece, piece), piece)
            give(k, 1, rr, inner[:, rows] + inner_part(k, xs, rows))

    def collect(k):
        for kind in range(GROUPS):
            takes = (
                jnp.where(is_last(k), 0, parity) == g
                if kind == 0
                else jnp.logical_not(is_last(k)) | (g == 1)
            )
            for src in range(GROUPS * R):

                @pl.when(takes & (src != me))
                def _():
                    remote(
                        pbuf.at[k, kind, src],
                        pbuf.at[k, kind, src],
                        y_s.at[0, 0],
                        y_r.at[k, kind, src],
                        {"row": r},
                    ).wait_recv()

            @pl.when(takes)
            def _():
                pbuf[k, kind, me] = psend[k, kind, r]
                total = pbuf[k, kind, 0]
                for src in range(1, GROUPS * R):
                    total = total + pbuf[k, kind, src]
                if kind == 1:
                    total = total * scales[:, pl.ds(pl.multiple_of(r * piece, piece), piece)]

                @pl.when(is_last(k))
                def _():
                    ubuf[...] = total

                @pl.when(jnp.logical_not(is_last(k)))
                def _():
                    trace = total.astype(BF)
                    tsend[k, kind] = trace
                    for dz in order:
                        if dz:
                            t_copy(k, kind, dz).start()
                    tbuf[k + 1, kind, z] = trace

        for way in range(3):
            for rr in range(R):

                @pl.when(y_other(k, way, rr))
                def _():
                    y_copy(k, way, rr).wait_send()

    def t_sent(k):
        for kind in range(GROUPS):

            @pl.when((kind == 1) | (parity == g))
            def _():
                for dz in order:
                    if dz:
                        t_copy(k, kind, dz).wait_send()

    acc[...] = outer_part(0, 0, everything)
    for xx in range(1, X - 1):
        acc[...] += outer_part(0, xx, everything)
    send_rows(0, X - 1)
    inner[...] = inner_part(0, 0, everything)
    for xx in range(1, X - 1):
        inner[...] += inner_part(0, xx, everything)
    inner_rows(0, X - 1)
    lax.fori_loop(0, X * GROUPS * GROUPS, make_gather, 0)
    collect(0)

    def iteration(k, carry):
        for zz in range(Z):

            @pl.when(zz != z)
            def _():
                remote(
                    tbuf.at[k, 1, zz], tbuf.at[k, 1, zz], t_s.at[0, 0], t_r.at[k, 1, zz], {"row": r}
                ).wait_recv()

        for zi in range(Zh):
            zs = GROUPS * zi + g

            @pl.when(zs != z)
            def _():
                remote(
                    tbuf.at[k, 0, zs], tbuf.at[k, 0, zs], t_s.at[0, 0], t_r.at[k, 0, zs], {"row": r}
                ).wait_recv()

        sources = []
        for j in range(GROUPS):
            for zz in range(GROUPS):
                source = tbuf[k, 1, zz].astype(F32)
                for n in range(1, Zh):
                    other = tbuf[k, 1, GROUPS * n + zz].astype(F32)
                    source = jnp.where(adj[j, s] == n, other, source)
                sources.append(source.astype(BF))
        for dx in x_order + [0]:
            xx = (x + dx) % X
            columns = pl.ds(pl.multiple_of(xx * piece, piece), piece)
            near = None
            for q, source in enumerate(sources):
                term = jnp.dot(source, gbuf[q, :, columns], preferred_element_type=F32)
                near = term if near is None else near + term
            nsend[k, xx] = near.astype(BF)
            if dx:
                n_copy(k, dx).start()

        for zi in range(Zh):
            zs = GROUPS * zi + g
            choice = metabuf[zs, 0:1, :]
            far = tbuf[k, 1, g].astype(F32)
            for n in range(1, Zh):
                far = jnp.where(choice == n, tbuf[k, 1, GROUPS * n + g].astype(F32), far)
            mixed = bbuf[0, zs].astype(F32) + robin_weight * (far - tbuf[k, 0, zs].astype(F32))
            we[k, x, zi] = mixed.astype(BF)
        for dx in x_order:
            we_copy(k, dx).start()

        acc[...] = outer_part(k, x, everything)

        near = nsend[k, x].astype(F32)
        for dx in range(1, X):
            xs = (x + dx) % X
            x_wait(nbuf.at[k, xs], k, 1, dx)
            near = near + nbuf[k, xs].astype(F32)
        own_inner = tbuf[k, 1, zt].astype(F32)
        own_outer = tbuf[k, 0, zt].astype(F32)
        mixed = (
            bbuf[1, zt].astype(F32)
            + robin_weight * (own_outer - own_inner)
            + iface_weight * (near - own_inner)
        )
        wi[k, x] = mixed.astype(BF)
        for dx in x_order:
            wi_copy(k, dx).start()

        x_near = x_order[::-1]
        for dx in x_near[:-1]:
            xs = (x + dx) % X
            x_wait(we.at[k, xs], k, 0, dx)
            acc[...] += outer_part(k, xs, everything)
        xs = (x + x_near[-1]) % X
        x_wait(we.at[k, xs], k, 0, x_near[-1])
        send_rows(k, xs)
        inner[...] = inner_part(k, x, everything)
        for dx in x_near[:-1]:
            xs = (x + dx) % X
            x_wait(wi.at[k, xs], k, 2, dx)
            inner[...] += inner_part(k, xs, everything)
        xs = (x + x_near[-1]) % X
        x_wait(wi.at[k, xs], k, 2, x_near[-1])
        inner_rows(k, xs)
        t_sent(k - 1)
        collect(k)
        for dx in x_order:
            we_copy(k, dx).wait_send()
            n_copy(k, dx).wait_send()
            wi_copy(k, dx).wait_send()
        return carry

    lax.fori_loop(1, ITERS, iteration, 0)
    out[0] = ubuf[...]


def body(
    excitation,
    panel_points,
    panel_areas,
    panel_map,
    interior_inverse,
    row_scales,
    iface_slot,
    iface_offset,
    adjacency,
):
    strips = lax.axis_size("col")
    R = lax.axis_size("row")
    _, rhs, piece = excitation.shape
    block = strips * piece
    sub_width = interior_inverse.shape[3]
    X = sub_width // (GROUPS * piece)
    Z = strips // X
    Zh = Z // GROUPS
    RP = R * piece
    P_ = X * Zh
    vm = pltpu.VMEM
    dma = pltpu.SemaphoreType.DMA
    in_vmem = pl.BlockSpec(memory_space=pltpu.VMEM)
    return pl.pallas_call(
        functools.partial(kernel, (Z, X, R, piece, block)),
        out_shape=jax.ShapeDtypeStruct((1, rhs, piece), F32),
        in_specs=[in_vmem] * 6
        + [pl.BlockSpec(memory_space=pltpu.SMEM), pl.BlockSpec(memory_space=pl.ANY), in_vmem],
        out_specs=in_vmem,
        scratch_shapes=[
            vm((3, KB, RP), F32),
            vm((16, P_ * piece), F32),
            vm((P_ * piece, 16), F32),
            vm((2, 9, KB, 128), F32),
            vm((X, Zh, piece, RP), BF),
            vm((RP, X * piece), BF),
            vm((GROUPS * GROUPS, piece, X * piece), BF),
            vm((8, piece), jnp.int32),
            vm((Z, 8, piece), jnp.int32),
            vm((X, 8, piece), jnp.int32),
            vm((GROUPS, Z, rhs, piece), BF),
            vm((ITERS, GROUPS, rhs, piece), BF),
            vm((ITERS, GROUPS, Z, rhs, piece), BF),
            vm((ITERS, X, Zh, rhs, piece), BF),
            vm((ITERS, X, rhs, piece), BF),
            vm((ITERS, X, rhs, piece), BF),
            vm((ITERS, X, rhs, piece), BF),
            vm((rhs, RP), F32),
            vm((rhs, RP), F32),
            vm((ITERS, GROUPS, R, rhs, piece), F32),
            vm((ITERS, GROUPS, GROUPS * R, rhs, piece), F32),
            vm((rhs, piece), F32),
            dma(()),
            dma((Z,)),
            dma((GROUPS, Z)),
            dma((Z,)),
            dma((Z,)),
            dma((GROUPS, Z)),
            dma((ITERS, GROUPS, Z)),
            dma((3, X)),
            dma((ITERS, 3, X)),
            dma((3, R)),
            dma((ITERS, GROUPS, GROUPS * R)),
        ],
        compiler_params=pltpu.CompilerParams(
            collective_id=0, has_side_effects=True, vmem_limit_bytes=60 * 1024 * 1024
        ),
    )(
        excitation,
        panel_points,
        panel_areas.reshape(1, -1),
        panel_map.reshape(1, -1),
        iface_slot.reshape(1, -1),
        iface_offset.reshape(1, -1),
        adjacency.T,
        interior_inverse[0, :, 0, :],
        row_scales,
    )


def solution(mesh):
    placed = (
        P("grp", None, ("row", "col")),
        P(),
        P(),
        P(("row", "col")),
        P("col", None, "row", None),
        P("col", None),
        P(("row", "col")),
        P(("row", "col")),
        P(),
    )
    return jax.shard_map(
        body, mesh=mesh, in_specs=placed, out_specs=P("grp", None, ("row", "col")), check_vma=False
    )
```

```python
import functools
import math

import jax
import jax.numpy as jnp
from jax import lax
from jax.experimental import pallas as pl
from jax.experimental.pallas import tpu as pltpu
from jax.sharding import PartitionSpec as P

ITERS = 4
GROUPS = 2
robin_weight = 0.5
iface_weight = 0.4
wave_number = 40.0
soften = 0.05
self_term = 0.5
KB = 32
X_CHIPS = 4

BF = jnp.bfloat16
F32 = jnp.float32
MESH = pl.DeviceIdType.MESH

COS_TERMS = (
    1.4142135381698608,
    -6.978850841522217,
    5.739460468292236,
    -1.883557915687561,
    0.3106880187988281,
)
TURNS = wave_number / (2.0 * math.pi)


def kernel(
    dims,
    exc,
    pts,
    areas,
    pmap,
    slot,
    off,
    adj,
    inv,
    scales,
    out,
    ipt,
    stage,
    kpt,
    kline,
    kbuf,
    abuf,
    gbuf,
    metasend,
    metabuf,
    xmeta,
    bbuf,
    tsend,
    tbuf,
    we,
    nsend,
    nbuf,
    wi,
    xtrace,
    acc,
    psend,
    pbuf,
    ubuf,
    asem,
    b_s,
    b_r,
    m_s,
    m_r,
    t_s,
    t_r,
    x_s,
    x_r,
    y_s,
    y_r,
):
    Z, X, R, piece, block = dims
    Zh = Z // GROUPS
    sub_width = GROUPS * X * piece
    RP = R * piece
    g = lax.axis_index("grp")
    r = lax.axis_index("row")
    c = lax.axis_index("col")
    z, x = c // X, c % X
    s = z // GROUPS
    zt = GROUPS * s + g
    parity = z % GROUPS
    me = g * R + r

    def remote(src, dst, ss, rs, dev):
        return pltpu.make_async_remote_copy(
            src_ref=src, dst_ref=dst, send_sem=ss, recv_sem=rs, device_id=dev, device_id_type=MESH
        )

    def col_of(zz, xx):
        return zz * X + xx

    barrier = pltpu.get_barrier_semaphore()
    n_partners = 0
    for flip in range(GROUPS):
        for dz in range(Z):
            if flip or dz:
                pl.semaphore_signal(
                    barrier,
                    inc=1,
                    device_id={"grp": (g + flip) % GROUPS, "row": r, "col": col_of((z + dz) % Z, x)},
                    device_id_type=MESH,
                )
                n_partners += 1
    for dx in range(1, X):
        pl.semaphore_signal(
            barrier,
            inc=1,
            device_id={"grp": g, "row": r, "col": col_of(z, (x + dx) % X)},
            device_id_type=MESH,
        )
        n_partners += 1
    for flip in range(GROUPS):
        for dr in range(1, R):
            pl.semaphore_signal(
                barrier,
                inc=1,
                device_id={"grp": (g + flip) % GROUPS, "row": (r + dr) % R, "col": c},
                device_id_type=MESH,
            )
            n_partners += 1

    inverse_copy = pltpu.make_async_copy(
        inv.at[:, pl.ds(pl.multiple_of(g * X * piece, X * piece), X * piece)], abuf, asem
    )
    inverse_copy.start()

    for rr in range(R):
        start = pl.multiple_of(rr * block + c * piece, piece)
        own = pts[:, pl.ds(start, piece)] * TURNS
        for axis in range(3):
            ipt[axis, :, rr * piece : (rr + 1) * piece] = jnp.broadcast_to(
                own[axis : axis + 1, :], (KB, piece)
            )
    for p in range(X * Zh):
        xx, zi = p // Zh, p % Zh
        start = pl.multiple_of(r * block + col_of(GROUPS * zi + g, xx) * piece, piece)
        lanes = slice(p * piece, (p + 1) * piece)
        stage[0:3, lanes] = pts[:, pl.ds(start, piece)] * TURNS
        area = areas[:, pl.ds(start, piece)] * TURNS
        stage[3:4, lanes] = area
        root = jnp.sqrt(area)
        for n, term in enumerate(COS_TERMS):
            stage[4 + n : 5 + n, lanes] = root * term
        stage[9:16, lanes] = jnp.zeros((7, piece), F32)
    kpt[...] = jnp.transpose(stage[...])

    per_piece = piece // KB
    last_block = X * Zh * per_piece - 1
    LANES = 128
    PAIR = min(RP, 2 * LANES)

    def spread(t, to):
        kc = kpt[pl.ds(pl.multiple_of(t * KB, KB), KB), :]
        for n in range(9):
            kline[to, n] = jnp.broadcast_to(kc[:, n : n + 1], (KB, LANES))

    spread(0, 0)

    def make_rows(t, carry):
        p = t // per_piece
        row = pl.multiple_of((t % per_piece) * KB, KB)
        now = t % 2
        for m in range(RP // PAIR):
            halves = []
            for half in range(PAIR // LANES):
                first = m * PAIR + half * LANES
                lanes = slice(first, first + LANES)
                dx = ipt[0, :, lanes] - kline[now, 0]
                dy = ipt[1, :, lanes] - kline[now, 1]
                dz = ipt[2, :, lanes] - kline[now, 2]
                square = dx * dx + dy * dy + dz * dz
                turns = 1.0 / lax.rsqrt(square)
                part = turns - jnp.round(turns)
                v = part * part
                h = kline[now, 8] * v + kline[now, 7]
                h = h * v + kline[now, 6]
                h = h * v + kline[now, 5]
                h = h * v + kline[now, 4]
                top = h * h - kline[now, 3]
                halves.append(top / (turns + soften * TURNS))
            value = jnp.concatenate(halves, axis=1).astype(BF)
            kbuf[p // Zh, p % Zh, pl.ds(row, KB), m * PAIR : (m + 1) * PAIR] = value
        spread(jnp.minimum(t + 1, last_block), 1 - now)
        return carry

    trips = X * Zh * per_piece
    cuts = (0, trips * 7 // 16, trips * 12 // 16, trips)

    def make_part(q):
        lax.fori_loop(cuts[q], cuts[q + 1], make_rows, 0)

    make_part(0)
    pl.semaphore_wait(barrier, n_partners)

    metasend[...] = jnp.zeros_like(metasend)
    metasend[0:1, :] = pmap[...]
    metasend[1:2, :] = slot[...] * sub_width + off[...]
    b_plane = parity

    def b_copy(dz):
        return remote(
            exc.at[0],
            bbuf.at[g, z],
            b_s.at[dz],
            b_r.at[g, z],
            {"grp": b_plane, "row": r, "col": col_of((z + dz) % Z, x)},
        )

    def m_copy(dz):
        return remote(
            metasend,
            metabuf.at[z],
            m_s.at[dz],
            m_r.at[z],
            {"grp": g, "row": r, "col": col_of((z + dz) % Z, x)},
        )

    order = sorted(range(Z), key=lambda dz: -min(dz, Z - dz))
    for dz in order:
        if dz:
            b_copy(dz).start()

            @pl.when(b_plane == g)
            def _():
                m_copy(dz).start()
        else:

            @pl.when(b_plane != g)
            def _():
                b_copy(0).start()

            @pl.when(b_plane == g)
            def _():
                bbuf[g, z] = exc[0]
                metabuf[z] = metasend[...]

    make_part(1)

    for zi in range(Zh):
        zs = GROUPS * zi + g
        for src in range(GROUPS):

            @pl.when((zs != z) | (g != src))
            def _():
                remote(
                    bbuf.at[src, zs], bbuf.at[src, zs], b_s.at[0], b_r.at[src, zs], {"row": r}
                ).wait_recv()

        @pl.when(zs != z)
        def _():
            remote(metabuf.at[zs], metabuf.at[zs], m_s.at[0], m_r.at[zs], {"row": r}).wait_recv()

    def x_dev(dx):
        return {"grp": g, "row": r, "col": col_of(z, (x + dx) % X)}

    x_order = sorted(range(1, X), key=lambda dx: -min(dx, X - dx))

    def we_copy(k, dx):
        return remote(we.at[k, x], we.at[k, x], x_s.at[0, dx], x_r.at[k, 0, x], x_dev(dx))

    def n_copy(k, dx):
        return remote(nsend.at[k], nbuf.at[k, x], x_s.at[1, dx], x_r.at[k, 1, x], x_dev(dx))

    def wi_copy(k, dx):
        return remote(wi.at[k, x], wi.at[k, x], x_s.at[2, dx], x_r.at[k, 2, x], x_dev(dx))

    def base_copy(k, kind, dx):
        return remote(
            tbuf.at[k, kind, zt],
            xtrace.at[k, kind, x],
            x_s.at[2 + kind, dx],
            x_r.at[k, 2 + kind, x],
            x_dev(dx),
        )

    def xm_copy(dx):
        return remote(metabuf.at[zt], xmeta.at[x], x_s.at[1, dx], x_r.at[0, 1, x], x_dev(dx))

    def x_wait(ref, k, kind, dx):
        xs = (x + dx) % X
        remote(ref, ref, x_s.at[kind, dx], x_r.at[k, kind, xs], x_dev(dx)).wait_recv()

    for zi in range(Zh):
        we[0, x, zi] = bbuf[0, GROUPS * zi + g]
    wi[0, x] = bbuf[1, zt]
    xmeta[x] = metabuf[zt]
    for dx in x_order:
        we_copy(0, dx).start()
        xm_copy(dx).start()
        wi_copy(0, dx).start()
    make_part(2)

    def make_gather(t, carry):
        xx, q = t // (GROUPS * GROUPS), t % (GROUPS * GROUPS)
        code = xmeta[xx, 1:2, :]
        src_x = (code // piece) % X
        src_q = code // (X * piece)
        here = jnp.where((src_x == x) & (src_q == q), code % piece, -1)
        rows = lax.broadcasted_iota(jnp.int32, (piece, piece), 0)
        hit = jnp.where(rows == here, 1.0, 0.0).astype(BF)
        gbuf[q, :, pl.ds(pl.multiple_of(xx * piece, piece), piece)] = hit
        return carry

    inverse_copy.wait()
    for dx in range(1, X):
        x_wait(we.at[0, (x + dx) % X], 0, 0, dx)
        x_wait(wi.at[0, (x + dx) % X], 0, 2, dx)
        x_wait(xmeta.at[(x + dx) % X], 0, 1, dx)
        we_copy(0, dx).wait_send()
        xm_copy(dx).wait_send()
        wi_copy(0, dx).wait_send()
    for dz in order:
        if dz:
            b_copy(dz).wait_send()

            @pl.when(b_plane == g)
            def _():
                m_copy(dz).wait_send()
        else:

            @pl.when(b_plane != g)
            def _():
                b_copy(0).wait_send()

    def is_last(k):
        return jnp.int32(k) == ITERS - 1

    def y_plane(k, way):
        return jnp.where(is_last(k), 0, parity) if way == 0 else 2 - way

    def y_copy(k, way, rr):
        kind = min(way, 1)
        return remote(
            psend.at[k, kind, rr],
            pbuf.at[k, kind, me],
            y_s.at[way, rr],
            y_r.at[k, kind, me],
            {"grp": y_plane(k, way), "row": rr, "col": c},
        )

    def y_other(k, way, rr):
        other = (g != y_plane(k, way)) | (r != rr)
        return other & jnp.logical_not(is_last(k)) if way == 2 else other

    def give(k, kind, rr, value):
        psend[k, kind, rr] = value
        for way in ((0,), (1, 2))[kind]:

            @pl.when(y_other(k, way, rr))
            def _():
                y_copy(k, way, rr).start()

    def t_copy(k, kind, dz):
        return remote(
            tsend.at[k, kind],
            tbuf.at[k + 1, kind, z],
            t_s.at[kind, dz],
            t_r.at[k + 1, kind, z],
            {"grp": g, "row": r, "col": col_of((z + dz) % Z, x)},
        )

    def outer_part(k, xs, columns):
        total = None
        for zi in range(Zh):
            term = jnp.dot(we[k, xs, zi], kbuf[xs, zi, :, columns], preferred_element_type=F32)
            total = term if total is None else total + term
        return total

    everything = slice(None)
    cores = min(R, 2)
    row_order = []
    for far in reversed(range(R // cores)):
        for side in reversed(range(cores)):
            row_order.append(
                ((r // cores + far) % (R // cores)) * cores + (r % cores + side) % cores
            )

    def send_rows(k, xs):
        for rr in row_order:
            columns = pl.ds(pl.multiple_of(rr * piece, piece), piece)
            value = acc[:, columns] + outer_part(k, xs, columns)
            own_piece = self_term * we[k, x, z // GROUPS].astype(F32)
            value = value + jnp.where((rr == r) & (parity == g), own_piece, 0.0)
            give(k, 0, rr, value)

    def inner_part(k, xs, rows):
        return lax.dot_general(
            wi[k, xs],
            abuf[rows, xs * piece : (xs + 1) * piece],
            (((1,), (1,)), ((), ())),
            preferred_element_type=F32,
        )

    def inner_rows(k, pieces):
        for rr in row_order:
            rows = pl.ds(pl.multiple_of(rr * piece, piece), piece)
            total = None
            for xs in pieces:
                term = inner_part(k, xs, rows)
                total = term if total is None else total + term
            give(k, 1, rr, total)

    def collect(k):
        for kind in range(GROUPS):
            takes = (
                jnp.where(is_last(k), 0, parity) == g
                if kind == 0
                else jnp.logical_not(is_last(k)) | (g == 1)
            )
            for src in range(GROUPS * R):

                @pl.when(takes & (src != me))
                def _():
                    remote(
                        pbuf.at[k, kind, src],
                        pbuf.at[k, kind, src],
                        y_s.at[0, 0],
                        y_r.at[k, kind, src],
                        {"row": r},
                    ).wait_recv()

            @pl.when(takes)
            def _():
                pbuf[k, kind, me] = psend[k, kind, r]
                total = pbuf[k, kind, 0]
                for src in range(1, GROUPS * R):
                    total = total + pbuf[k, kind, src]
                if kind == 1:
                    total = total * scales[:, pl.ds(pl.multiple_of(r * piece, piece), piece)]

                @pl.when(is_last(k))
                def _():
                    ubuf[...] = total

                @pl.when(jnp.logical_not(is_last(k)))
                def _():
                    trace = total.astype(BF)
                    tsend[k, kind] = trace
                    for dz in order:
                        if dz:
                            t_copy(k, kind, dz).start()
                    tbuf[k + 1, kind, z] = trace

        for way in range(3):
            for rr in range(R):

                @pl.when(y_other(k, way, rr))
                def _():
                    y_copy(k, way, rr).wait_send()

    def t_sent(k):
        for kind in range(GROUPS):

            @pl.when((kind == 1) | (parity == g))
            def _():
                for dz in order:
                    if dz:
                        t_copy(k, kind, dz).wait_send()

    acc[...] = outer_part(0, 0, everything)
    for xx in range(1, X - 1):
        acc[...] += outer_part(0, xx, everything)
    send_rows(0, X - 1)
    inner_rows(0, range(X))
    lax.fori_loop(0, X * GROUPS * GROUPS, make_gather, 0)
    collect(0)

    def iteration(k, carry):
        for zz in range(Z):

            @pl.when(zz != z)
            def _():
                remote(
                    tbuf.at[k, 1, zz], tbuf.at[k, 1, zz], t_s.at[0, 0], t_r.at[k, 1, zz], {"row": r}
                ).wait_recv()

        for zi in range(Zh):
            zs = GROUPS * zi + g

            @pl.when(zs != z)
            def _():
                remote(
                    tbuf.at[k, 0, zs], tbuf.at[k, 0, zs], t_s.at[0, 0], t_r.at[k, 0, zs], {"row": r}
                ).wait_recv()

        for zi in range(Zh):
            zs = GROUPS * zi + g
            choice = metabuf[zs, 0:1, :]
            far = tbuf[k, 1, g].astype(F32)
            for n in range(1, Zh):
                far = jnp.where(choice == n, tbuf[k, 1, GROUPS * n + g].astype(F32), far)
            mixed = bbuf[0, zs].astype(F32) + robin_weight * (far - tbuf[k, 0, zs].astype(F32))
            we[k, x, zi] = mixed.astype(BF)
        for dx in x_order:
            we_copy(k, dx).start()

        for dx in x_order:
            for kind in range(GROUPS):
                base_copy(k, kind, dx).start()
        sources = []
        for j in range(GROUPS):
            for zz in range(GROUPS):
                source = tbuf[k, 1, zz].astype(F32)
                for n in range(1, Zh):
                    other = tbuf[k, 1, GROUPS * n + zz].astype(F32)
                    source = jnp.where(adj[j, s] == n, other, source)
                sources.append(source.astype(BF))
        for xx in range(X):
            columns = slice(xx * piece, (xx + 1) * piece)
            near = None
            for q, source in enumerate(sources):
                term = jnp.dot(source, gbuf[q, :, columns], preferred_element_type=F32)
                near = term if near is None else near + term
            nsend[k, xx] = near.astype(BF)
        for dx in x_order:
            n_copy(k, dx).start()

        acc[...] = outer_part(k, x, everything)

        x_near = x_order[::-1]
        for dx in x_near[:-1]:
            xs = (x + dx) % X
            x_wait(we.at[k, xs], k, 0, dx)
            acc[...] += outer_part(k, xs, everything)
        xs = (x + x_near[-1]) % X
        x_wait(we.at[k, xs], k, 0, x_near[-1])
        send_rows(k, xs)
        for dx in x_near:
            xs = (x + dx) % X
            x_wait(nbuf.at[k, xs], k, 1, dx)
            for kind in range(GROUPS):
                x_wait(xtrace.at[k, kind, xs], k, 2 + kind, dx)
        for dx in range(X):
            xs = (x + dx) % X
            near = nsend[k, xs].astype(F32)
            for other in range(1, X):
                near = near + nbuf[k, (x + other) % X, xs].astype(F32)
            own_outer = (xtrace[k, 0, xs] if dx else tbuf[k, 0, zt]).astype(F32)
            own_inner = (xtrace[k, 1, xs] if dx else tbuf[k, 1, zt]).astype(F32)
            mixed = (
                wi[0, xs].astype(F32)
                + robin_weight * (own_outer - own_inner)
                + iface_weight * (near - own_inner)
            )
            wi[k, xs] = mixed.astype(BF)
        inner_rows(k, range(X))
        t_sent(k - 1)
        collect(k)
        for dx in x_order:
            we_copy(k, dx).wait_send()
            n_copy(k, dx).wait_send()
            for kind in range(GROUPS):
                base_copy(k, kind, dx).wait_send()
        return carry

    lax.fori_loop(1, ITERS, iteration, 0)
    out[0] = ubuf[...]


def body(
    excitation,
    panel_points,
    panel_areas,
    panel_map,
    interior_inverse,
    row_scales,
    iface_slot,
    iface_offset,
    adjacency,
):
    strips = lax.axis_size("col")
    R = lax.axis_size("row")
    _, rhs, piece = excitation.shape
    block = strips * piece
    sub_width = interior_inverse.shape[3]
    X = sub_width // (GROUPS * piece)
    Z = strips // X
    Zh = Z // GROUPS
    RP = R * piece
    P_ = X * Zh
    vm = pltpu.VMEM
    dma = pltpu.SemaphoreType.DMA
    in_vmem = pl.BlockSpec(memory_space=pltpu.VMEM)
    return pl.pallas_call(
        functools.partial(kernel, (Z, X, R, piece, block)),
        out_shape=jax.ShapeDtypeStruct((1, rhs, piece), F32),
        in_specs=[in_vmem] * 6
        + [pl.BlockSpec(memory_space=pltpu.SMEM), pl.BlockSpec(memory_space=pl.ANY), in_vmem],
        out_specs=in_vmem,
        scratch_shapes=[
            vm((3, KB, RP), F32),
            vm((16, P_ * piece), F32),
            vm((P_ * piece, 16), F32),
            vm((2, 9, KB, 128), F32),
            vm((X, Zh, piece, RP), BF),
            vm((RP, X * piece), BF),
            vm((GROUPS * GROUPS, piece, X * piece), BF),
            vm((8, piece), jnp.int32),
            vm((Z, 8, piece), jnp.int32),
            vm((X, 8, piece), jnp.int32),
            vm((GROUPS, Z, rhs, piece), BF),
            vm((ITERS, GROUPS, rhs, piece), BF),
            vm((ITERS, GROUPS, Z, rhs, piece), BF),
            vm((ITERS, X, Zh, rhs, piece), BF),
            vm((ITERS, X, rhs, piece), BF),
            vm((ITERS, X, X, rhs, piece), BF),
            vm((ITERS, X, rhs, piece), BF),
            vm((ITERS, GROUPS, X, rhs, piece), BF),
            vm((rhs, RP), F32),
            vm((ITERS, GROUPS, R, rhs, piece), F32),
            vm((ITERS, GROUPS, GROUPS * R, rhs, piece), F32),
            vm((rhs, piece), F32),
            dma(()),
            dma((Z,)),
            dma((GROUPS, Z)),
            dma((Z,)),
            dma((Z,)),
            dma((GROUPS, Z)),
            dma((ITERS, GROUPS, Z)),
            dma((4, X)),
            dma((ITERS, 4, X)),
            dma((3, R)),
            dma((ITERS, GROUPS, GROUPS * R)),
        ],
        compiler_params=pltpu.CompilerParams(
            collective_id=0, has_side_effects=True, vmem_limit_bytes=60 * 1024 * 1024
        ),
    )(
        excitation,
        panel_points,
        panel_areas.reshape(1, -1),
        panel_map.reshape(1, -1),
        iface_slot.reshape(1, -1),
        iface_offset.reshape(1, -1),
        adjacency.T,
        interior_inverse[0, :, 0, :],
        row_scales,
    )


def solution(mesh):
    placed = (
        P("grp", None, ("row", "col")),
        P(),
        P(),
        P(("row", "col")),
        P("col", None, "row", None),
        P("col", None),
        P(("row", "col")),
        P(("row", "col")),
        P(),
    )
    return jax.shard_map(
        body, mesh=mesh, in_specs=placed, out_specs=P("grp", None, ("row", "col")), check_vma=False
    )
```

```python
import functools
import math

import jax
import jax.numpy as jnp
from jax import lax
from jax.experimental import pallas as pl
from jax.experimental.pallas import tpu as pltpu
from jax.sharding import PartitionSpec as P

ITERS = 4
GROUPS = 2
robin_weight = 0.5
iface_weight = 0.4
wave_number = 40.0
soften = 0.05
self_term = 0.5
KB = 32
X_CHIPS = 4

BF = jnp.bfloat16
F32 = jnp.float32
MESH = pl.DeviceIdType.MESH

COS_TERMS = (
    1.4142135381698608,
    -6.978850841522217,
    5.739460468292236,
    -1.883557915687561,
    0.3106880187988281,
)
TURNS = wave_number / (2.0 * math.pi)


def kernel(
    dims,
    exc,
    pts,
    areas,
    pmap,
    slot,
    off,
    adj,
    inv,
    scales,
    out,
    ipt,
    stage,
    kpt,
    kline,
    kbuf,
    abuf,
    gbuf,
    metasend,
    metabuf,
    xmeta,
    bbuf,
    tsend,
    tbuf,
    we,
    nsend,
    nbuf,
    wi,
    xtrace,
    acc,
    psend,
    pbuf,
    asem,
    b_s,
    b_r,
    m_s,
    m_r,
    t_s,
    t_r,
    x_s,
    x_r,
    y_s,
    y_r,
):
    Z, X, R, piece, block = dims
    Zh = Z // GROUPS
    sub_width = GROUPS * X * piece
    RP = R * piece
    g = lax.axis_index("grp")
    r = lax.axis_index("row")
    c = lax.axis_index("col")
    z, x = c // X, c % X
    s = z // GROUPS
    zt = GROUPS * s + g
    parity = z % GROUPS
    me = g * R + r

    def remote(src, dst, ss, rs, dev):
        return pltpu.make_async_remote_copy(
            src_ref=src, dst_ref=dst, send_sem=ss, recv_sem=rs, device_id=dev, device_id_type=MESH
        )

    def col_of(zz, xx):
        return zz * X + xx

    barrier = pltpu.get_barrier_semaphore()
    n_partners = 0
    for flip in range(GROUPS):
        for dz in range(Z):
            if flip or dz:
                pl.semaphore_signal(
                    barrier,
                    inc=1,
                    device_id={"grp": (g + flip) % GROUPS, "row": r, "col": col_of((z + dz) % Z, x)},
                    device_id_type=MESH,
                )
                n_partners += 1
    for dx in range(1, X):
        pl.semaphore_signal(
            barrier,
            inc=1,
            device_id={"grp": g, "row": r, "col": col_of(z, (x + dx) % X)},
            device_id_type=MESH,
        )
        n_partners += 1
    for flip in range(GROUPS):
        for dr in range(1, R):
            pl.semaphore_signal(
                barrier,
                inc=1,
                device_id={"grp": (g + flip) % GROUPS, "row": (r + dr) % R, "col": c},
                device_id_type=MESH,
            )
            n_partners += 1

    inverse_copy = pltpu.make_async_copy(
        inv.at[:, pl.ds(pl.multiple_of(g * X * piece, X * piece), X * piece)], abuf, asem
    )
    inverse_copy.start()

    for rr in range(R):
        start = pl.multiple_of(rr * block + c * piece, piece)
        own = pts[:, pl.ds(start, piece)] * TURNS
        for axis in range(3):
            ipt[axis, :, rr * piece : (rr + 1) * piece] = jnp.broadcast_to(
                own[axis : axis + 1, :], (KB, piece)
            )
    for p in range(X * Zh):
        xx, zi = p // Zh, p % Zh
        start = pl.multiple_of(r * block + col_of(GROUPS * zi + g, xx) * piece, piece)
        lanes = slice(p * piece, (p + 1) * piece)
        stage[0:3, lanes] = pts[:, pl.ds(start, piece)] * TURNS
        area = areas[:, pl.ds(start, piece)] * TURNS
        stage[3:4, lanes] = area
        root = jnp.sqrt(area)
        for n, term in enumerate(COS_TERMS):
            stage[4 + n : 5 + n, lanes] = root * term
        stage[9:16, lanes] = jnp.zeros((7, piece), F32)
    kpt[...] = jnp.transpose(stage[...])

    per_piece = piece // KB
    last_block = X * Zh * per_piece - 1
    LANES = 128
    PAIR = min(RP, 2 * LANES)

    def spread(t, to):
        kc = kpt[pl.ds(pl.multiple_of(t * KB, KB), KB), :]
        for n in range(9):
            kline[to, n] = jnp.broadcast_to(kc[:, n : n + 1], (KB, LANES))

    spread(0, 0)

    def make_rows(t, carry):
        p = t // per_piece
        row = pl.multiple_of((t % per_piece) * KB, KB)
        now = t % 2
        for m in range(RP // PAIR):
            halves = []
            for half in range(PAIR // LANES):
                first = m * PAIR + half * LANES
                lanes = slice(first, first + LANES)
                dx = ipt[0, :, lanes] - kline[now, 0]
                dy = ipt[1, :, lanes] - kline[now, 1]
                dz = ipt[2, :, lanes] - kline[now, 2]
                square = dx * dx + dy * dy + dz * dz
                turns = 1.0 / lax.rsqrt(square)
                part = turns - jnp.round(turns)
                v = part * part
                h = kline[now, 8] * v + kline[now, 7]
                h = h * v + kline[now, 6]
                h = h * v + kline[now, 5]
                h = h * v + kline[now, 4]
                top = h * h - kline[now, 3]
                halves.append(top / (turns + soften * TURNS))
            value = jnp.concatenate(halves, axis=1).astype(BF)
            kbuf[p // Zh, p % Zh, pl.ds(row, KB), m * PAIR : (m + 1) * PAIR] = value
        spread(jnp.minimum(t + 1, last_block), 1 - now)
        return carry

    trips = X * Zh * per_piece
    cuts = (0, trips * 7 // 16, trips * 12 // 16, trips)

    def make_part(q):
        lax.fori_loop(cuts[q], cuts[q + 1], make_rows, 0)

    make_part(0)
    pl.semaphore_wait(barrier, n_partners)

    metasend[...] = jnp.zeros_like(metasend)
    metasend[0:1, :] = pmap[...]
    metasend[1:2, :] = slot[...] * sub_width + off[...]
    b_plane = parity

    def b_copy(dz):
        return remote(
            exc.at[0],
            bbuf.at[g, z],
            b_s.at[dz],
            b_r.at[g, z],
            {"grp": b_plane, "row": r, "col": col_of((z + dz) % Z, x)},
        )

    def m_copy(dz):
        return remote(
            metasend,
            metabuf.at[z],
            m_s.at[dz],
            m_r.at[z],
            {"grp": g, "row": r, "col": col_of((z + dz) % Z, x)},
        )

    order = sorted(range(Z), key=lambda dz: -min(dz, Z - dz))
    for dz in order:
        if dz:
            b_copy(dz).start()

            @pl.when(b_plane == g)
            def _():
                m_copy(dz).start()
        else:

            @pl.when(b_plane != g)
            def _():
                b_copy(0).start()

            @pl.when(b_plane == g)
            def _():
                bbuf[g, z] = exc[0]
                metabuf[z] = metasend[...]

    make_part(1)

    for zi in range(Zh):
        zs = GROUPS * zi + g
        for src in range(GROUPS):

            @pl.when((zs != z) | (g != src))
            def _():
                remote(
                    bbuf.at[src, zs], bbuf.at[src, zs], b_s.at[0], b_r.at[src, zs], {"row": r}
                ).wait_recv()

        @pl.when(zs != z)
        def _():
            remote(metabuf.at[zs], metabuf.at[zs], m_s.at[0], m_r.at[zs], {"row": r}).wait_recv()

    def x_dev(dx):
        return {"grp": g, "row": r, "col": col_of(z, (x + dx) % X)}

    x_order = sorted(range(1, X), key=lambda dx: -min(dx, X - dx))

    def we_copy(k, dx):
        return remote(we.at[k, x], we.at[k, x], x_s.at[0, dx], x_r.at[k, 0, x], x_dev(dx))

    def n_copy(k, dx):
        return remote(nsend.at[k], nbuf.at[k, x], x_s.at[1, dx], x_r.at[k, 1, x], x_dev(dx))

    def wi_copy(k, dx):
        return remote(wi.at[k, x], wi.at[k, x], x_s.at[2, dx], x_r.at[k, 2, x], x_dev(dx))

    def base_copy(k, kind, dx):
        return remote(
            tbuf.at[k, kind, zt],
            xtrace.at[k, kind, x],
            x_s.at[2 + kind, dx],
            x_r.at[k, 2 + kind, x],
            x_dev(dx),
        )

    def xm_copy(dx):
        return remote(metabuf.at[zt], xmeta.at[x], x_s.at[1, dx], x_r.at[0, 1, x], x_dev(dx))

    def x_wait(ref, k, kind, dx):
        xs = (x + dx) % X
        remote(ref, ref, x_s.at[kind, dx], x_r.at[k, kind, xs], x_dev(dx)).wait_recv()

    for zi in range(Zh):
        we[0, x, zi] = bbuf[0, GROUPS * zi + g]
    wi[0, x] = bbuf[1, zt]
    xmeta[x] = metabuf[zt]
    for dx in x_order:
        we_copy(0, dx).start()
        xm_copy(dx).start()
        wi_copy(0, dx).start()
    make_part(2)

    def make_gather(t, carry):
        xx, q = t // (GROUPS * GROUPS), t % (GROUPS * GROUPS)
        code = xmeta[xx, 1:2, :]
        src_x = (code // piece) % X
        src_q = code // (X * piece)
        here = jnp.where((src_x == x) & (src_q == q), code % piece, -1)
        rows = lax.broadcasted_iota(jnp.int32, (piece, piece), 0)
        hit = jnp.where(rows == here, 1.0, 0.0).astype(BF)
        gbuf[q, :, pl.ds(pl.multiple_of(xx * piece, piece), piece)] = hit
        return carry

    inverse_copy.wait()
    for dx in range(1, X):
        x_wait(we.at[0, (x + dx) % X], 0, 0, dx)
        x_wait(wi.at[0, (x + dx) % X], 0, 2, dx)
        x_wait(xmeta.at[(x + dx) % X], 0, 1, dx)

    def is_last(k):
        return jnp.int32(k) == ITERS - 1

    def y_plane(k, way):
        return jnp.where(is_last(k), 0, parity) if way == 0 else 2 - way

    def y_copy(k, way, rr):
        kind = min(way, 1)
        return remote(
            psend.at[k, kind, rr],
            pbuf.at[k, kind, me],
            y_s.at[way, rr],
            y_r.at[k, kind, me],
            {"grp": y_plane(k, way), "row": rr, "col": c},
        )

    def y_other(k, way, rr):
        other = (g != y_plane(k, way)) | (r != rr)
        return other & jnp.logical_not(is_last(k)) if way == 2 else other

    def give(k, kind, rr, value):
        psend[k, kind, rr] = value
        for way in ((0,), (1, 2))[kind]:

            @pl.when(y_other(k, way, rr))
            def _():
                y_copy(k, way, rr).start()

    def t_copy(k, kind, dz):
        return remote(
            tsend.at[k, kind],
            tbuf.at[k + 1, kind, z],
            t_s.at[kind, dz],
            t_r.at[k + 1, kind, z],
            {"grp": g, "row": r, "col": col_of((z + dz) % Z, x)},
        )

    def outer_part(k, xs, columns):
        total = None
        for zi in range(Zh):
            term = jnp.dot(we[k, xs, zi], kbuf[xs, zi, :, columns], preferred_element_type=F32)
            total = term if total is None else total + term
        return total

    everything = slice(None)
    cores = min(R, 2)
    row_order = []
    for far in reversed(range(R // cores)):
        for side in reversed(range(cores)):
            row_order.append(
                ((r // cores + far) % (R // cores)) * cores + (r % cores + side) % cores
            )

    def send_rows(k, xs):
        for rr in row_order:
            columns = pl.ds(pl.multiple_of(rr * piece, piece), piece)
            value = acc[:, columns] + outer_part(k, xs, columns)
            own_piece = self_term * we[k, x, z // GROUPS].astype(F32)
            value = value + jnp.where((rr == r) & (parity == g), own_piece, 0.0)
            give(k, 0, rr, value)

    def inner_part(k, xs, rows):
        return lax.dot_general(
            wi[k, xs],
            abuf[rows, xs * piece : (xs + 1) * piece],
            (((1,), (1,)), ((), ())),
            preferred_element_type=F32,
        )

    def inner_rows(k, pieces):
        for rr in row_order:
            rows = pl.ds(pl.multiple_of(rr * piece, piece), piece)
            total = None
            for xs in pieces:
                term = inner_part(k, xs, rows)
                total = term if total is None else total + term
            give(k, 1, rr, total)

    def collect(k):
        for kind in range(GROUPS):
            takes = (
                jnp.where(is_last(k), 0, parity) == g
                if kind == 0
                else jnp.logical_not(is_last(k)) | (g == 1)
            )
            for src in range(GROUPS * R):

                @pl.when(takes & (src != me))
                def _():
                    remote(
                        pbuf.at[k, kind, src],
                        pbuf.at[k, kind, src],
                        y_s.at[0, 0],
                        y_r.at[k, kind, src],
                        {"row": r},
                    ).wait_recv()

            @pl.when(takes)
            def _():
                pbuf[k, kind, me] = psend[k, kind, r]
                total = pbuf[k, kind, 0]
                for src in range(1, GROUPS * R):
                    total = total + pbuf[k, kind, src]
                if kind == 1:
                    total = total * scales[:, pl.ds(pl.multiple_of(r * piece, piece), piece)]

                @pl.when(is_last(k))
                def _():
                    out[0] = total

                @pl.when(jnp.logical_not(is_last(k)))
                def _():
                    trace = total.astype(BF)
                    tsend[k, kind] = trace
                    for dz in order:
                        if dz:
                            t_copy(k, kind, dz).start()
                    tbuf[k + 1, kind, z] = trace

        for way in range(3):
            for rr in range(R):

                @pl.when(y_other(k, way, rr))
                def _():
                    y_copy(k, way, rr).wait_send()

    def t_sent(k):
        for kind in range(GROUPS):

            @pl.when((kind == 1) | (parity == g))
            def _():
                for dz in order:
                    if dz:
                        t_copy(k, kind, dz).wait_send()

    acc[...] = outer_part(0, 0, everything)
    for xx in range(1, X - 1):
        acc[...] += outer_part(0, xx, everything)
    send_rows(0, X - 1)
    inner_rows(0, range(X))
    for dx in range(1, X):
        we_copy(0, dx).wait_send()
        xm_copy(dx).wait_send()
        wi_copy(0, dx).wait_send()
    for dz in order:
        if dz:
            b_copy(dz).wait_send()

            @pl.when(b_plane == g)
            def _():
                m_copy(dz).wait_send()
        else:

            @pl.when(b_plane != g)
            def _():
                b_copy(0).wait_send()
    lax.fori_loop(0, X * GROUPS * GROUPS, make_gather, 0)
    collect(0)

    def iteration(k, carry):
        for zi in range(Zh):
            zs = GROUPS * zi + g

            @pl.when(zs != z)
            def _():
                remote(
                    tbuf.at[k, 0, zs], tbuf.at[k, 0, zs], t_s.at[0, 0], t_r.at[k, 0, zs], {"row": r}
                ).wait_recv()

        for zi in range(Zh):
            zs = GROUPS * zi + g

            @pl.when(zs != z)
            def _():
                remote(
                    tbuf.at[k, 1, zs], tbuf.at[k, 1, zs], t_s.at[0, 0], t_r.at[k, 1, zs], {"row": r}
                ).wait_recv()

        for zi in range(Zh):
            zs = GROUPS * zi + g
            choice = metabuf[zs, 0:1, :]
            far = tbuf[k, 1, g].astype(F32)
            for n in range(1, Zh):
                far = jnp.where(choice == n, tbuf[k, 1, GROUPS * n + g].astype(F32), far)
            mixed = bbuf[0, zs].astype(F32) + robin_weight * (far - tbuf[k, 0, zs].astype(F32))
            we[k, x, zi] = mixed.astype(BF)
        for dx in x_order:
            we_copy(k, dx).start()

        for zi in range(Zh):
            zs = GROUPS * zi + (1 - g)

            @pl.when(zs != z)
            def _():
                remote(
                    tbuf.at[k, 1, zs], tbuf.at[k, 1, zs], t_s.at[0, 0], t_r.at[k, 1, zs], {"row": r}
                ).wait_recv()

        sources = []
        for j in range(GROUPS):
            for zz in range(GROUPS):
                source = tbuf[k, 1, zz].astype(F32)
                for n in range(1, Zh):
                    other = tbuf[k, 1, GROUPS * n + zz].astype(F32)
                    source = jnp.where(adj[j, s] == n, other, source)
                sources.append(source.astype(BF))
        for xx in range(X):
            columns = slice(xx * piece, (xx + 1) * piece)
            near = None
            for q, source in enumerate(sources):
                term = jnp.dot(source, gbuf[q, :, columns], preferred_element_type=F32)
                near = term if near is None else near + term
            nsend[k, xx] = near.astype(BF)
        for dx in x_order:
            n_copy(k, dx).start()
        for dx in x_order:
            for kind in range(GROUPS):
                base_copy(k, kind, dx).start()

        acc[...] = outer_part(k, x, everything)

        x_near = x_order[::-1]
        for dx in x_near[:-1]:
            xs = (x + dx) % X
            x_wait(we.at[k, xs], k, 0, dx)
            acc[...] += outer_part(k, xs, everything)
        xs = (x + x_near[-1]) % X
        x_wait(we.at[k, xs], k, 0, x_near[-1])
        send_rows(k, xs)
        for dx in x_near:
            xs = (x + dx) % X
            x_wait(nbuf.at[k, xs], k, 1, dx)
            for kind in range(GROUPS):
                x_wait(xtrace.at[k, kind, xs], k, 2 + kind, dx)
        for dx in range(X):
            xs = (x + dx) % X
            near = nsend[k, xs].astype(F32)
            for other in range(1, X):
                near = near + nbuf[k, (x + other) % X, xs].astype(F32)
            own_outer = (xtrace[k, 0, xs] if dx else tbuf[k, 0, zt]).astype(F32)
            own_inner = (xtrace[k, 1, xs] if dx else tbuf[k, 1, zt]).astype(F32)
            mixed = (
                wi[0, xs].astype(F32)
                + robin_weight * (own_outer - own_inner)
                + iface_weight * (near - own_inner)
            )
            wi[k, xs] = mixed.astype(BF)
        inner_rows(k, range(X))
        t_sent(k - 1)
        collect(k)
        for dx in x_order:
            we_copy(k, dx).wait_send()
            n_copy(k, dx).wait_send()
            for kind in range(GROUPS):
                base_copy(k, kind, dx).wait_send()
        return carry

    lax.fori_loop(1, ITERS, iteration, 0)


def body(
    excitation,
    panel_points,
    panel_areas,
    panel_map,
    interior_inverse,
    row_scales,
    iface_slot,
    iface_offset,
    adjacency,
):
    strips = lax.axis_size("col")
    R = lax.axis_size("row")
    _, rhs, piece = excitation.shape
    block = strips * piece
    sub_width = interior_inverse.shape[3]
    X = sub_width // (GROUPS * piece)
    Z = strips // X
    Zh = Z // GROUPS
    RP = R * piece
    P_ = X * Zh
    vm = pltpu.VMEM
    dma = pltpu.SemaphoreType.DMA
    in_vmem = pl.BlockSpec(memory_space=pltpu.VMEM)
    return pl.pallas_call(
        functools.partial(kernel, (Z, X, R, piece, block)),
        out_shape=jax.ShapeDtypeStruct((1, rhs, piece), F32),
        in_specs=[in_vmem] * 6
        + [pl.BlockSpec(memory_space=pltpu.SMEM), pl.BlockSpec(memory_space=pl.ANY), in_vmem],
        out_specs=in_vmem,
        scratch_shapes=[
            vm((3, KB, RP), F32),
            vm((16, P_ * piece), F32),
            vm((P_ * piece, 16), F32),
            vm((2, 9, KB, 128), F32),
            vm((X, Zh, piece, RP), BF),
            vm((RP, X * piece), BF),
            vm((GROUPS * GROUPS, piece, X * piece), BF),
            vm((8, piece), jnp.int32),
            vm((Z, 8, piece), jnp.int32),
            vm((X, 8, piece), jnp.int32),
            vm((GROUPS, Z, rhs, piece), BF),
            vm((ITERS, GROUPS, rhs, piece), BF),
            vm((ITERS, GROUPS, Z, rhs, piece), BF),
            vm((ITERS, X, Zh, rhs, piece), BF),
            vm((ITERS, X, rhs, piece), BF),
            vm((ITERS, X, X, rhs, piece), BF),
            vm((ITERS, X, rhs, piece), BF),
            vm((ITERS, GROUPS, X, rhs, piece), BF),
            vm((rhs, RP), F32),
            vm((ITERS, GROUPS, R, rhs, piece), F32),
            vm((ITERS, GROUPS, GROUPS * R, rhs, piece), F32),
            dma(()),
            dma((Z,)),
            dma((GROUPS, Z)),
            dma((Z,)),
            dma((Z,)),
            dma((GROUPS, Z)),
            dma((ITERS, GROUPS, Z)),
            dma((4, X)),
            dma((ITERS, 4, X)),
            dma((3, R)),
            dma((ITERS, GROUPS, GROUPS * R)),
        ],
        compiler_params=pltpu.CompilerParams(
            collective_id=0, has_side_effects=True, vmem_limit_bytes=60 * 1024 * 1024
        ),
    )(
        excitation,
        panel_points,
        panel_areas.reshape(1, -1),
        panel_map.reshape(1, -1),
        iface_slot.reshape(1, -1),
        iface_offset.reshape(1, -1),
        adjacency.T,
        interior_inverse[0, :, 0, :],
        row_scales,
    )


def solution(mesh):
    placed = (
        P("grp", None, ("row", "col")),
        P(),
        P(),
        P(("row", "col")),
        P("col", None, "row", None),
        P("col", None),
        P(("row", "col")),
        P(("row", "col")),
        P(),
    )
    return jax.shard_map(
        body, mesh=mesh, in_specs=placed, out_specs=P("grp", None, ("row", "col")), check_vma=False
    )
```

```python
import functools
import math

import jax
import jax.numpy as jnp
from jax import lax
from jax.experimental import pallas as pl
from jax.experimental.pallas import tpu as pltpu
from jax.sharding import PartitionSpec as P

ITERS = 4
GROUPS = 2
robin_weight = 0.5
iface_weight = 0.4
wave_number = 40.0
soften = 0.05
self_term = 0.5
KB = 32
X_CHIPS = 4

BF = jnp.bfloat16
F32 = jnp.float32
MESH = pl.DeviceIdType.MESH

COS_TERMS = (
    1.4142135381698608,
    -6.978850841522217,
    5.739460468292236,
    -1.883557915687561,
    0.3106880187988281,
)
TURNS = wave_number / (2.0 * math.pi)


def kernel(
    dims,
    exc,
    pts,
    areas,
    pmap,
    slot,
    off,
    adj,
    inv,
    scales,
    out,
    ipt,
    stage,
    kpt,
    kline,
    kbuf,
    abuf,
    gbuf,
    metasend,
    metabuf,
    xmeta,
    bbuf,
    tsend,
    tbuf,
    we,
    nsend,
    nbuf,
    wi,
    xtrace,
    acc,
    psend,
    pbuf,
    asem,
    b_s,
    b_r,
    m_s,
    m_r,
    t_s,
    t_r,
    x_s,
    x_r,
    y_s,
    y_r,
):
    Z, X, R, piece, block = dims
    Zh = Z // GROUPS
    sub_width = GROUPS * X * piece
    RP = R * piece
    g = lax.axis_index("grp")
    r = lax.axis_index("row")
    c = lax.axis_index("col")
    z, x = c // X, c % X
    s = z // GROUPS
    zt = GROUPS * s + g
    parity = z % GROUPS
    me = g * R + r

    def remote(src, dst, ss, rs, dev):
        return pltpu.make_async_remote_copy(
            src_ref=src, dst_ref=dst, send_sem=ss, recv_sem=rs, device_id=dev, device_id_type=MESH
        )

    def col_of(zz, xx):
        return zz * X + xx

    barrier = pltpu.get_barrier_semaphore()
    n_partners = 0
    for flip in range(GROUPS):
        for dz in range(Z):
            if flip or dz:
                pl.semaphore_signal(
                    barrier,
                    inc=1,
                    device_id={"grp": (g + flip) % GROUPS, "row": r, "col": col_of((z + dz) % Z, x)},
                    device_id_type=MESH,
                )
                n_partners += 1
    for dx in range(1, X):
        pl.semaphore_signal(
            barrier,
            inc=1,
            device_id={"grp": g, "row": r, "col": col_of(z, (x + dx) % X)},
            device_id_type=MESH,
        )
        n_partners += 1
    for flip in range(GROUPS):
        for dr in range(1, R):
            pl.semaphore_signal(
                barrier,
                inc=1,
                device_id={"grp": (g + flip) % GROUPS, "row": (r + dr) % R, "col": c},
                device_id_type=MESH,
            )
            n_partners += 1

    inverse_copy = pltpu.make_async_copy(
        inv.at[:, pl.ds(pl.multiple_of(g * X * piece, X * piece), X * piece)], abuf, asem
    )
    inverse_copy.start()

    for rr in range(R):
        start = pl.multiple_of(rr * block + c * piece, piece)
        own = pts[:, pl.ds(start, piece)] * TURNS
        for axis in range(3):
            ipt[axis, :, rr * piece : (rr + 1) * piece] = jnp.broadcast_to(
                own[axis : axis + 1, :], (KB, piece)
            )
    for p in range(X * Zh):
        xx, zi = p // Zh, p % Zh
        start = pl.multiple_of(r * block + col_of(GROUPS * zi + g, xx) * piece, piece)
        lanes = slice(p * piece, (p + 1) * piece)
        stage[0:3, lanes] = pts[:, pl.ds(start, piece)] * TURNS
        area = areas[:, pl.ds(start, piece)] * TURNS
        stage[3:4, lanes] = area
        root = jnp.sqrt(area)
        for n, term in enumerate(COS_TERMS):
            stage[4 + n : 5 + n, lanes] = root * term
        stage[9:16, lanes] = jnp.zeros((7, piece), F32)
    kpt[...] = jnp.transpose(stage[...])

    per_piece = piece // KB
    last_block = X * Zh * per_piece - 1
    LANES = 128
    PAIR = min(RP, 2 * LANES)

    def spread(t, to):
        kc = kpt[pl.ds(pl.multiple_of(t * KB, KB), KB), :]
        for n in range(9):
            kline[to, n] = jnp.broadcast_to(kc[:, n : n + 1], (KB, LANES))

    spread(0, 0)

    def make_rows(t, carry):
        p = t // per_piece
        row = pl.multiple_of((t % per_piece) * KB, KB)
        now = t % 2
        for m in range(RP // PAIR):
            halves = []
            for half in range(PAIR // LANES):
                first = m * PAIR + half * LANES
                lanes = slice(first, first + LANES)
                dx = ipt[0, :, lanes] - kline[now, 0]
                dy = ipt[1, :, lanes] - kline[now, 1]
                dz = ipt[2, :, lanes] - kline[now, 2]
                square = dx * dx + dy * dy + dz * dz
                turns = 1.0 / lax.rsqrt(square)
                part = turns - jnp.round(turns)
                v = part * part
                h = kline[now, 8] * v + kline[now, 7]
                h = h * v + kline[now, 6]
                h = h * v + kline[now, 5]
                h = h * v + kline[now, 4]
                top = h * h - kline[now, 3]
                halves.append(top / (turns + soften * TURNS))
            value = jnp.concatenate(halves, axis=1).astype(BF)
            kbuf[p // Zh, p % Zh, pl.ds(row, KB), m * PAIR : (m + 1) * PAIR] = value
        spread(jnp.minimum(t + 1, last_block), 1 - now)
        return carry

    trips = X * Zh * per_piece
    cuts = (0, trips * 7 // 16, trips * 12 // 16, trips)

    def make_part(q):
        lax.fori_loop(cuts[q], cuts[q + 1], make_rows, 0)

    make_part(0)
    pl.semaphore_wait(barrier, n_partners)

    metasend[...] = jnp.zeros_like(metasend)
    metasend[0:1, :] = pmap[...]
    metasend[1:2, :] = slot[...] * sub_width + off[...]
    b_plane = parity

    def b_copy(dz):
        return remote(
            exc.at[0],
            bbuf.at[g, z],
            b_s.at[dz],
            b_r.at[g, z],
            {"grp": b_plane, "row": r, "col": col_of((z + dz) % Z, x)},
        )

    def m_copy(dz):
        return remote(
            metasend,
            metabuf.at[z],
            m_s.at[dz],
            m_r.at[z],
            {"grp": g, "row": r, "col": col_of((z + dz) % Z, x)},
        )

    order = sorted(range(Z), key=lambda dz: -min(dz, Z - dz))
    for dz in order:
        if dz:
            b_copy(dz).start()

            @pl.when(b_plane == g)
            def _():
                m_copy(dz).start()
        else:

            @pl.when(b_plane != g)
            def _():
                b_copy(0).start()

            @pl.when(b_plane == g)
            def _():
                bbuf[g, z] = exc[0]
                metabuf[z] = metasend[...]

    make_part(1)

    for zi in range(Zh):
        zs = GROUPS * zi + g
        for src in range(GROUPS):

            @pl.when((zs != z) | (g != src))
            def _():
                remote(
                    bbuf.at[src, zs], bbuf.at[src, zs], b_s.at[0], b_r.at[src, zs], {"row": r}
                ).wait_recv()

        @pl.when(zs != z)
        def _():
            remote(metabuf.at[zs], metabuf.at[zs], m_s.at[0], m_r.at[zs], {"row": r}).wait_recv()

    def x_dev(dx):
        return {"grp": g, "row": r, "col": col_of(z, (x + dx) % X)}

    x_order = sorted(range(1, X), key=lambda dx: -min(dx, X - dx))

    def we_copy(k, dx):
        return remote(we.at[k, x], we.at[k, x], x_s.at[0, dx], x_r.at[k, 0, x], x_dev(dx))

    def n_copy(k, dx):
        return remote(nsend.at[k], nbuf.at[k, x], x_s.at[1, dx], x_r.at[k, 1, x], x_dev(dx))

    def wi_copy(k, dx):
        return remote(wi.at[k, x], wi.at[k, x], x_s.at[2, dx], x_r.at[k, 2, x], x_dev(dx))

    def base_copy(k, kind, dx):
        return remote(
            tbuf.at[k, kind, zt],
            xtrace.at[k, kind, x],
            x_s.at[2 + kind, dx],
            x_r.at[k, 2 + kind, x],
            x_dev(dx),
        )

    def xm_copy(dx):
        return remote(metabuf.at[zt], xmeta.at[x], x_s.at[1, dx], x_r.at[0, 1, x], x_dev(dx))

    def x_wait(ref, k, kind, dx):
        xs = (x + dx) % X
        remote(ref, ref, x_s.at[kind, dx], x_r.at[k, kind, xs], x_dev(dx)).wait_recv()

    for zi in range(Zh):
        we[0, x, zi] = bbuf[0, GROUPS * zi + g]
    wi[0, x] = bbuf[1, zt]
    xmeta[x] = metabuf[zt]
    for dx in x_order:
        we_copy(0, dx).start()
        xm_copy(dx).start()
        wi_copy(0, dx).start()
    make_part(2)

    def make_gather(t, carry):
        xx, q = t // (GROUPS * GROUPS), t % (GROUPS * GROUPS)
        code = xmeta[xx, 1:2, :]
        src_x = (code // piece) % X
        src_q = code // (X * piece)
        here = jnp.where((src_x == x) & (src_q == q), code % piece, -1)
        rows = lax.broadcasted_iota(jnp.int32, (piece, piece), 0)
        hit = jnp.where(rows == here, 1.0, 0.0).astype(BF)
        gbuf[q, :, pl.ds(pl.multiple_of(xx * piece, piece), piece)] = hit
        return carry

    inverse_copy.wait()
    for dx in range(1, X):
        x_wait(we.at[0, (x + dx) % X], 0, 0, dx)
        x_wait(wi.at[0, (x + dx) % X], 0, 2, dx)
        x_wait(xmeta.at[(x + dx) % X], 0, 1, dx)

    def is_last(k):
        return jnp.int32(k) == ITERS - 1

    def y_plane(k, way):
        return jnp.where(is_last(k), 0, parity) if way == 0 else 2 - way

    def y_copy(k, way, rr):
        kind = min(way, 1)
        return remote(
            psend.at[k, kind, rr],
            pbuf.at[k, kind, me],
            y_s.at[way, rr],
            y_r.at[k, kind, me],
            {"grp": y_plane(k, way), "row": rr, "col": c},
        )

    def y_other(k, way, rr):
        other = (g != y_plane(k, way)) | (r != rr)
        return other & jnp.logical_not(is_last(k)) if way == 2 else other

    def give(k, kind, rr, value):
        psend[k, kind, rr] = value
        for way in ((0,), (1, 2))[kind]:

            @pl.when(y_other(k, way, rr))
            def _():
                y_copy(k, way, rr).start()

    def t_copy(k, kind, dz):
        return remote(
            tsend.at[k, kind],
            tbuf.at[k + 1, kind, z],
            t_s.at[kind, dz],
            t_r.at[k + 1, kind, z],
            {"grp": g, "row": r, "col": col_of((z + dz) % Z, x)},
        )

    def outer_part(k, xs, columns):
        total = None
        for zi in range(Zh):
            term = jnp.dot(we[k, xs, zi], kbuf[xs, zi, :, columns], preferred_element_type=F32)
            total = term if total is None else total + term
        return total

    everything = slice(None)
    cores = min(R, 2)
    row_order = []
    for far in reversed(range(R // cores)):
        for side in reversed(range(cores)):
            row_order.append(
                ((r // cores + far) % (R // cores)) * cores + (r % cores + side) % cores
            )

    def send_rows(k, xs):
        for rr in row_order:
            columns = pl.ds(pl.multiple_of(rr * piece, piece), piece)
            value = acc[:, columns] + outer_part(k, xs, columns)
            own_piece = self_term * we[k, x, z // GROUPS].astype(F32)
            value = value + jnp.where((rr == r) & (parity == g), own_piece, 0.0)
            give(k, 0, rr, value)

    def inner_part(k, xs, rows):
        return lax.dot_general(
            wi[k, xs],
            abuf[rows, xs * piece : (xs + 1) * piece],
            (((1,), (1,)), ((), ())),
            preferred_element_type=F32,
        )

    def inner_rows(k, pieces):
        for rr in row_order:
            rows = pl.ds(pl.multiple_of(rr * piece, piece), piece)
            total = None
            for xs in pieces:
                term = inner_part(k, xs, rows)
                total = term if total is None else total + term
            give(k, 1, rr, total)

    def collect(k):
        for kind in range(GROUPS):
            takes = (
                jnp.where(is_last(k), 0, parity) == g
                if kind == 0
                else jnp.logical_not(is_last(k)) | (g == 1)
            )
            @pl.when(takes)
            def _():
                pbuf[k, kind, me] = psend[k, kind, r]
                for step in range(1, GROUPS * R):
                    src = (me + step) % (GROUPS * R)
                    landed = pbuf.at[k, kind, src]
                    remote(landed, landed, y_s.at[0, 0], y_r.at[k, kind, src], {"row": r}).wait_recv()
                total = pbuf[k, kind, 0]
                for src in range(1, GROUPS * R):
                    total = total + pbuf[k, kind, src]
                if kind == 1:
                    total = total * scales[:, pl.ds(pl.multiple_of(r * piece, piece), piece)]

                @pl.when(is_last(k))
                def _():
                    out[0] = total

                @pl.when(jnp.logical_not(is_last(k)))
                def _():
                    trace = total.astype(BF)
                    tsend[k, kind] = trace
                    for dz in order:
                        if dz:
                            t_copy(k, kind, dz).start()
                    tbuf[k + 1, kind, z] = trace

        for way in range(3):
            for rr in range(R):

                @pl.when(y_other(k, way, rr))
                def _():
                    y_copy(k, way, rr).wait_send()

    def t_sent(k):
        for kind in range(GROUPS):

            @pl.when((kind == 1) | (parity == g))
            def _():
                for dz in order:
                    if dz:
                        t_copy(k, kind, dz).wait_send()

    acc[...] = outer_part(0, 0, everything)
    for xx in range(1, X - 1):
        acc[...] += outer_part(0, xx, everything)
    send_rows(0, X - 1)
    inner_rows(0, range(X))
    for dx in range(1, X):
        we_copy(0, dx).wait_send()
        xm_copy(dx).wait_send()
        wi_copy(0, dx).wait_send()
    for dz in order:
        if dz:
            b_copy(dz).wait_send()

            @pl.when(b_plane == g)
            def _():
                m_copy(dz).wait_send()
        else:

            @pl.when(b_plane != g)
            def _():
                b_copy(0).wait_send()
    lax.fori_loop(0, X * GROUPS * GROUPS, make_gather, 0)
    collect(0)

    def iteration(k, carry):
        shift = jnp.where(parity == g, 0, 1)
        for zi in range(Zh):
            zs = (z + GROUPS * zi + shift) % Z

            def arrive(zs=zs):
                for kind in (0, 1):
                    landed = tbuf.at[k, kind, zs]
                    remote(landed, landed, t_s.at[0, 0], t_r.at[k, kind, zs], {"row": r}).wait_recv()

            if zi:
                arrive()
            else:
                pl.when(shift != 0)(arrive)

        for zi in range(Zh):
            zs = GROUPS * zi + g
            choice = metabuf[zs, 0:1, :]
            far = tbuf[k, 1, g].astype(F32)
            for n in range(1, Zh):
                far = jnp.where(choice == n, tbuf[k, 1, GROUPS * n + g].astype(F32), far)
            mixed = bbuf[0, zs].astype(F32) + robin_weight * (far - tbuf[k, 0, zs].astype(F32))
            we[k, x, zi] = mixed.astype(BF)
        for dx in x_order:
            we_copy(k, dx).start()

        shift = jnp.where(parity == g, 1, 0)
        for zi in range(Zh):
            zs = (z + GROUPS * zi + shift) % Z

            def arrive(zs=zs):
                for kind in (1,):
                    landed = tbuf.at[k, kind, zs]
                    remote(landed, landed, t_s.at[0, 0], t_r.at[k, kind, zs], {"row": r}).wait_recv()

            if zi:
                arrive()
            else:
                pl.when(shift != 0)(arrive)

        sources = []
        for j in range(GROUPS):
            for zz in range(GROUPS):
                source = tbuf[k, 1, zz].astype(F32)
                for n in range(1, Zh):
                    other = tbuf[k, 1, GROUPS * n + zz].astype(F32)
                    source = jnp.where(adj[j, s] == n, other, source)
                sources.append(source.astype(BF))
        for xx in range(X):
            columns = slice(xx * piece, (xx + 1) * piece)
            near = None
            for q, source in enumerate(sources):
                term = jnp.dot(source, gbuf[q, :, columns], preferred_element_type=F32)
                near = term if near is None else near + term
            nsend[k, xx] = near.astype(BF)
        for dx in x_order:
            n_copy(k, dx).start()
        for dx in x_order:
            for kind in range(GROUPS):
                base_copy(k, kind, dx).start()

        acc[...] = outer_part(k, x, everything)

        x_near = x_order[::-1]
        for dx in x_near[:-1]:
            xs = (x + dx) % X
            x_wait(we.at[k, xs], k, 0, dx)
            acc[...] += outer_part(k, xs, everything)
        xs = (x + x_near[-1]) % X
        x_wait(we.at[k, xs], k, 0, x_near[-1])
        send_rows(k, xs)
        for dx in x_near:
            xs = (x + dx) % X
            x_wait(nbuf.at[k, xs], k, 1, dx)
            for kind in range(GROUPS):
                x_wait(xtrace.at[k, kind, xs], k, 2 + kind, dx)
        for dx in range(X):
            xs = (x + dx) % X
            near = nsend[k, xs].astype(F32)
            for other in range(1, X):
                near = near + nbuf[k, (x + other) % X, xs].astype(F32)
            own_outer = (xtrace[k, 0, xs] if dx else tbuf[k, 0, zt]).astype(F32)
            own_inner = (xtrace[k, 1, xs] if dx else tbuf[k, 1, zt]).astype(F32)
            mixed = (
                wi[0, xs].astype(F32)
                + robin_weight * (own_outer - own_inner)
                + iface_weight * (near - own_inner)
            )
            wi[k, xs] = mixed.astype(BF)
        inner_rows(k, range(X))
        t_sent(k - 1)
        collect(k)
        for dx in x_order:
            we_copy(k, dx).wait_send()
            n_copy(k, dx).wait_send()
            for kind in range(GROUPS):
                base_copy(k, kind, dx).wait_send()
        return carry

    lax.fori_loop(1, ITERS, iteration, 0)


def body(
    excitation,
    panel_points,
    panel_areas,
    panel_map,
    interior_inverse,
    row_scales,
    iface_slot,
    iface_offset,
    adjacency,
):
    strips = lax.axis_size("col")
    R = lax.axis_size("row")
    _, rhs, piece = excitation.shape
    block = strips * piece
    sub_width = interior_inverse.shape[3]
    X = sub_width // (GROUPS * piece)
    Z = strips // X
    Zh = Z // GROUPS
    RP = R * piece
    P_ = X * Zh
    vm = pltpu.VMEM
    dma = pltpu.SemaphoreType.DMA
    in_vmem = pl.BlockSpec(memory_space=pltpu.VMEM)
    return pl.pallas_call(
        functools.partial(kernel, (Z, X, R, piece, block)),
        out_shape=jax.ShapeDtypeStruct((1, rhs, piece), F32),
        in_specs=[in_vmem] * 6
        + [pl.BlockSpec(memory_space=pltpu.SMEM), pl.BlockSpec(memory_space=pl.ANY), in_vmem],
        out_specs=in_vmem,
        scratch_shapes=[
            vm((3, KB, RP), F32),
            vm((16, P_ * piece), F32),
            vm((P_ * piece, 16), F32),
            vm((2, 9, KB, 128), F32),
            vm((X, Zh, piece, RP), BF),
            vm((RP, X * piece), BF),
            vm((GROUPS * GROUPS, piece, X * piece), BF),
            vm((8, piece), jnp.int32),
            vm((Z, 8, piece), jnp.int32),
            vm((X, 8, piece), jnp.int32),
            vm((GROUPS, Z, rhs, piece), BF),
            vm((ITERS, GROUPS, rhs, piece), BF),
            vm((ITERS, GROUPS, Z, rhs, piece), BF),
            vm((ITERS, X, Zh, rhs, piece), BF),
            vm((ITERS, X, rhs, piece), BF),
            vm((ITERS, X, X, rhs, piece), BF),
            vm((ITERS, X, rhs, piece), BF),
            vm((ITERS, GROUPS, X, rhs, piece), BF),
            vm((rhs, RP), F32),
            vm((ITERS, GROUPS, R, rhs, piece), F32),
            vm((ITERS, GROUPS, GROUPS * R, rhs, piece), F32),
            dma(()),
            dma((Z,)),
            dma((GROUPS, Z)),
            dma((Z,)),
            dma((Z,)),
            dma((GROUPS, Z)),
            dma((ITERS, GROUPS, Z)),
            dma((4, X)),
            dma((ITERS, 4, X)),
            dma((3, R)),
            dma((ITERS, GROUPS, GROUPS * R)),
        ],
        compiler_params=pltpu.CompilerParams(
            collective_id=0, has_side_effects=True, vmem_limit_bytes=60 * 1024 * 1024
        ),
    )(
        excitation,
        panel_points,
        panel_areas.reshape(1, -1),
        panel_map.reshape(1, -1),
        iface_slot.reshape(1, -1),
        iface_offset.reshape(1, -1),
        adjacency.T,
        interior_inverse[0, :, 0, :],
        row_scales,
    )


def solution(mesh):
    placed = (
        P("grp", None, ("row", "col")),
        P(),
        P(),
        P(("row", "col")),
        P("col", None, "row", None),
        P("col", None),
        P(("row", "col")),
        P(("row", "col")),
        P(),
    )
    return jax.shard_map(
        body, mesh=mesh, in_specs=placed, out_specs=P("grp", None, ("row", "col")), check_vma=False
    )
```
